512 devices in a mesh: row: 32 (over z, x), col: 16 (over y, core).
Axes of the slice: x: 4, y: 8, z: 8, core: 2. Of those that a mesh axis runs over, the one named last changes fastest.
Arguments:
- lower: bfloat16 [32, 3, 512, 2, 512], P('row', None, None, None, 'col'), as said below
- rhs: bfloat16 [32, 3, 512, 8192], P('row', None, None, 'col'), may hold values from -6 to 6
- tile_map: int32 [16], replicated, may hold values from 0 to 15, each once
Outputs:
- overwritten: bfloat16 [32, 3, 512, 8192], P('row', None, None, 'col')
The draws below stay inside these ranges and needn't reach their ends.
Inputs may be any that keep to these rules, and one draw needn't show every extreme that they name: tile_map is a permutation of 0 to 15. lower[0, 0, :, 0, :] and lower[1, 0, :, 1, :] are lower triangular with diagonal entries between 2 and 3; lower[0, 0, :, 1, :] is zero.
All inputs are finite; a program needn't handle non-finite values.
Results may differ from the reference program's by a relative error of at most 0.0032.
Values may be sent and summed in bfloat16 or wider, within the bound.
A program may use at most 64 MiB of HBM per device.

```python
import jax
import jax.numpy as jnp

TB = 512
R = 8192
MT = 3
RT = 16
N_ROW = 32


def draw_lower(key, part):
    keys = jax.random.split(jax.random.fold_in(key, 11), 6)
    shape = (N_ROW, MT, TB, 2, TB)
    base = jax.random.normal(keys[0], shape, jnp.float32)
    base = base * TB ** (-0.5)
    for panel in range(2):
        strict = jax.random.normal(keys[1 + panel], (TB, TB), jnp.float32)
        strict = jnp.tril(strict * 0.8 * TB ** (-0.5), -1)
        values = jax.random.uniform(keys[3 + panel], (TB,), jnp.float32, 2.0, 3.0)
        base = base.at[panel, 0, :, panel, :].set(strict + jnp.diag(values))
    base = base.at[0, 0, :, 1, :].set(0.0)
    return base.astype(jnp.bfloat16)


def block_levels(rng, shape, cuts, smallest, top_value):
    def one(dim, blocks):
        draws = jax.random.uniform(jax.random.fold_in(jax.random.fold_in(rng, 6), dim), (blocks,), jnp.float32, smallest / len(cuts), top_value / len(cuts))
        return jnp.repeat(jnp.exp(draws), shape[dim] // blocks).reshape((-1,) + (1,) * (len(shape) - dim - 1))

    level = one(*cuts[0])
    for cut in cuts[1:]:
        level = level * one(*cut)
    return level


def noise(rng, extent, spread, most, cuts=(), kind=jnp.bfloat16):
    drawn = spread * jax.random.normal(rng, extent, jnp.float32)
    if cuts:
        drawn = drawn * block_levels(rng, extent, cuts, -0.22, 0.18)
    return jnp.clip(drawn, -most, most).astype(kind)


def setup_inputs(seed: int = 0) -> dict:
    arg_keys = jax.random.split(jax.random.key(seed), 4)
    lower = draw_lower(jax.random.fold_in(arg_keys[3], 71), 0)
    rhs = noise(arg_keys[1], (N_ROW, MT, TB, R), 1.0, 6.0, ((0, 32), (3, 16)))
    tile_map = jax.random.permutation(arg_keys[2], RT).astype(jnp.int32)
    return {"lower": lower, "rhs": rhs, "tile_map": tile_map}


def redistribute(array, tile_map):
    shape = array.shape
    tiles = array.reshape(shape[:-1] + (RT, TB))
    return jnp.take(tiles, tile_map, axis=3).reshape(shape)

def reference(lower, rhs, tile_map):
    work = rhs.astype(jnp.float32)
    solved_rows = []
    for panel in range(2):
        diagonal = jnp.tril(lower[panel, 0, :, panel, :].astype(jnp.float32))
        solved = jax.scipy.linalg.solve_triangular(diagonal, work[panel, 0], lower=True).astype(jnp.bfloat16)
        flat = lower[:, :, :, panel, :].reshape(N_ROW * MT * TB, TB)
        update = jnp.dot(flat.astype(jnp.float32), solved.astype(jnp.float32), preferred_element_type=jnp.float32)
        work = work - update.reshape(work.shape)
        solved_rows.append(solved)
    result = work.astype(jnp.bfloat16)
    result = result.at[0, 0].set(solved_rows[0])
    result = result.at[1, 0].set(solved_rows[1])
    return redistribute(result, tile_map)
```

```python
import functools

import jax
import jax.numpy as jnp
from jax import lax
from jax.experimental import pallas as pl
from jax.experimental.pallas import tpu as pltpu
from jax.sharding import PartitionSpec as P

MESH = pl.DeviceIdType.MESH
BLOCK = 128
HIGHEST = lax.Precision.HIGHEST


def dot_t(a, b):
    return lax.dot_general(a, b, (((0,), (0,)), ((), ())), preferred_element_type=jnp.float32)


def dot_f32(a, b):
    return jnp.dot(a, b, preferred_element_type=jnp.float32, precision=HIGHEST)


def kernel(
    rows, cols, tm_ref, rhs_ref, lt_ref, out_ref,
    a0, a1, a2, t0, t1, t2, c_ref, g_ref, s0_ref, s1_ref, acc_ref, lf_ref, inv_ref, x_ref,
    p1_send, p1_recv, p2_send, p2_recv, up_send, up_recv, down_send, down_recv,
    pair_send, pair_recv, sc_send, sc_recv, ga_send, ga_recv,
):
    a_refs, t_refs = (a0, a1, a2), (t0, t1, t2)
    tiles, tile = rhs_ref.shape[0], rhs_ref.shape[1]
    slab, piece = tile // cols, tile // rows
    chips = cols // 2
    far = chips // 2
    blocks = tile // BLOCK
    row, col = lax.axis_index("row"), lax.axis_index("col")
    chip, core = col // 2, col % 2

    barrier = pltpu.get_barrier_semaphore()

    def greet_col(d, _):
        pl.semaphore_signal(
            barrier, inc=1, device_id={"col": lax.rem(col + d, cols)}, device_id_type=MESH
        )
        return 0

    def greet_row(d, _):
        pl.semaphore_signal(
            barrier, inc=1, device_id={"row": lax.rem(row + d, rows)}, device_id_type=MESH
        )
        return 0

    lax.fori_loop(1, cols, greet_col, 0)
    lax.fori_loop(1, rows, greet_row, 0)
    pl.semaphore_wait(barrier, cols + rows - 2)

    def at_chip(offset):
        return lax.rem(chip + offset + 2 * chips, chips) * 2 + core

    def rows_of(index, size):
        return pl.ds(pl.multiple_of(index * size, size), size)

    def remote(src, dst, send, recv, target):
        copy = pltpu.make_async_remote_copy(
            src_ref=src, dst_ref=dst, send_sem=send, recv_sem=recv,
            device_id=target, device_id_type=MESH,
        )
        copy.start()

    def drain(ref, sem):
        pltpu.make_async_copy(ref, ref, sem).wait()

    partner = {"col": chip * 2 + 1 - core}

    def panel(offset, half=None):
        where = rows_of(at_chip(offset), slab)
        if half is None:
            return g_ref.at[:, :, where, :]
        return g_ref.at[:, half, where, :]

    def send_up(step):
        half = 0 if step == far else None
        block = panel(1 - step, half)
        src = lt_ref if step == 1 else block
        if step == 1 and half is not None:
            src = lt_ref.at[:, half]
        remote(src, block, up_send.at[step - 1], up_recv.at[step - 1], {"col": at_chip(1)})

    def send_down(step):
        half = 1 if step == far else None
        block = panel(step - 1, half)
        src = lt_ref if step == 1 else block
        if step == 1 and half is not None:
            src = lt_ref.at[:, half]
        remote(src, block, down_send.at[step - 1], down_recv.at[step - 1], {"col": at_chip(-1)})

    def arrive(step):
        up = panel(-step, 0 if step == far else None)
        down = panel(step, 1 if step == far else None)
        drain(up, up_recv.at[step - 1])
        drain(down, down_recv.at[step - 1])
        if step < far:
            send_up(step + 1)
            send_down(step + 1)
        remote(up, up, pair_send, pair_recv, partner)
        remote(down, down, pair_send, pair_recv, partner)

    order = []
    for d in range(far, 0, -1):
        order += [d] if d in (far,) else [d, chips - d]
    targets = []
    for d in order:
        targets.append(lax.rem(chip + d, chips) * 2 + core)
        targets.append(lax.rem(chip + d, chips) * 2 + 1 - core)
    targets.append(chip * 2 + 1 - core)

    def phase1(m):
        for p in targets:
            remote(
                rhs_ref.at[m, rows_of(p, slab), :], a_refs[m].at[col],
                p1_send.at[m], p1_recv.at[m], {"col": p},
            )
        a_refs[m][col] = rhs_ref[m, rows_of(col, slab), :]

    def phase2(m):
        drain(a_refs[m].at[pl.ds(0, cols - 1)], p1_recv.at[m])
        for j in range(cols):
            t_refs[m][j] = a_refs[m][tm_ref[j]]
        c_ref[m, rows_of(col, slab), :] = t_refs[m][col]
        for p in targets:
            remote(
                t_refs[m].at[p], c_ref.at[m, rows_of(col, slab), :],
                p2_send.at[m], p2_recv.at[m], {"col": p},
            )

    def phase2_done(m):
        drain(t_refs[m].at[pl.ds(0, cols - 1)], p2_recv.at[m])

    def invert(k):
        for i in range(blocks):
            for j in range(i + 1):
                u = g_ref[0, k, j * BLOCK : (j + 1) * BLOCK, i * BLOCK : (i + 1) * BLOCK]
                lf_ref[i * BLOCK : (i + 1) * BLOCK, j * BLOCK : (j + 1) * BLOCK] = (
                    u.astype(jnp.float32).T
                )
        r = lax.broadcasted_iota(jnp.int32, (BLOCK, BLOCK), 0)
        c = lax.broadcasted_iota(jnp.int32, (BLOCK, BLOCK), 1)
        eye = r == c
        diag = [
            lf_ref[i * BLOCK : (i + 1) * BLOCK, i * BLOCK : (i + 1) * BLOCK]
            for i in range(blocks)
        ]
        xs = [jnp.where(eye, 1.0 / jnp.where(eye, d, 1.0), 0.0) for d in diag]
        shift = 0
        while (1 << shift) < BLOCK:
            rb, cb = r >> shift, c >> shift
            mask = ((rb >> 1) == (cb >> 1)) & (rb > cb)
            mids = [dot_f32(x, jnp.where(mask, d, 0.0)) for x, d in zip(xs, diag)]
            xs = [x - dot_f32(mid, x) for x, mid in zip(xs, mids)]
            shift += 1
        for i in range(blocks):
            inv_ref[i] = xs[i]

    def solve(work, s_ref):
        for i in range(blocks):
            rng = slice(i * BLOCK, (i + 1) * BLOCK)
            r = work(rng)
            if i:
                r = r - dot_f32(lf_ref[rng, : i * BLOCK], x_ref[: i * BLOCK, :])
            x = dot_f32(inv_ref[i], r)
            x_ref[rng, :] = x
            s_ref[rng, :] = x.astype(jnp.bfloat16)

    def scatter(root, k, s_ref):
        def one(d, _):
            p = lax.rem(row + d, rows)
            remote(
                s_ref.at[rows_of(p, piece), :], s_ref.at[rows_of(p, piece), :],
                sc_send.at[k], sc_recv.at[k], {"row": p},
            )
            return 0

        lax.fori_loop(1, rows, one, 0)

    def gather(root, k, s_ref):
        @pl.when(row != root)
        def _():
            drain(s_ref.at[pl.ds(0, piece), :], sc_recv.at[k])

        mine = s_ref.at[rows_of(row, piece), :]

        def one(d, _):
            p = lax.rem(row + d, rows)

            @pl.when(p != root)
            def _():
                remote(mine, mine, ga_send.at[k], ga_recv.at[k], {"row": p})

            return 0

        lax.fori_loop(1, rows, one, 0)

    def gathered(root, k, s_ref):
        @pl.when(row != root)
        def _():
            drain(s_ref.at[pl.ds(0, tile - piece), :], ga_recv.at[k])

    def update(k, s_ref):
        def one(step, _):
            m, at = step // blocks, step % blocks
            cut = pl.ds(pl.multiple_of(at * BLOCK, BLOCK), BLOCK)
            term = dot_t(g_ref[m, k, :, cut], s_ref[...])
            if k == 0:
                acc_ref[m, cut, :] = term
            else:
                acc_ref[m, cut, :] = acc_ref[m, cut, :] + term
            return 0

        lax.fori_loop(0, tiles * blocks, one, 0)

    send_up(1)
    send_down(1)
    remote(lt_ref, panel(0), pair_send, pair_recv, partner)
    g_ref[:, :, rows_of(col, slab), :] = lt_ref[...]
    phase1(0)
    for step in range(1, far):
        arrive(step)
    phase1(1)
    phase2(0)
    phase1(2)
    arrive(far)
    drain(g_ref.at[:, :, pl.ds(0, tile // 2), :], pair_recv)

    @pl.when(row == 0)
    def _():
        invert(0)

    @pl.when(row == 1)
    def _():
        invert(1)

    phase2(1)
    phase2_done(0)

    @pl.when(row == 0)
    def _():
        solve(lambda rng: c_ref[0, rng, :].astype(jnp.float32), s0_ref)
        scatter(0, 0, s0_ref)

    gather(0, 0, s0_ref)
    phase2(2)
    gathered(0, 0, s0_ref)
    update(0, s0_ref)

    @pl.when(row == 1)
    def _():
        solve(lambda rng: c_ref[0, rng, :].astype(jnp.float32) - acc_ref[0, rng, :], s1_ref)
        scatter(1, 1, s1_ref)

    gather(1, 1, s1_ref)
    gathered(1, 1, s1_ref)
    update(1, s1_ref)

    for m in range(tiles):
        if m:
            phase2_done(m)
        out_ref[m] = (c_ref[m].astype(jnp.float32) - acc_ref[m]).astype(jnp.bfloat16)

    @pl.when(row == 0)
    def _():
        out_ref[0] = s0_ref[...]

    @pl.when(row == 1)
    def _():
        out_ref[0] = s1_ref[...]

    for step in range(1, far + 1):
        drain(panel(0, 0 if step == far else None), up_send.at[step - 1])
        drain(panel(0, 1 if step == far else None), down_send.at[step - 1])
    drain(g_ref.at[:, :, pl.ds(0, tile // 2), :], pair_send)
    for m in range(tiles):
        drain(a_refs[m].at[pl.ds(0, cols - 1)], p1_send.at[m])
        drain(t_refs[m].at[pl.ds(0, cols - 1)], p2_send.at[m])
    for k, (root, s_ref) in enumerate(((0, s0_ref), (1, s1_ref))):
        @pl.when(row == root)
        def _():
            drain(s_ref.at[pl.ds(0, tile - piece), :], sc_send.at[k])
            drain(s_ref.at[pl.ds(0, tile - piece), :], ga_send.at[k])

        @pl.when(row != root)
        def _():
            drain(s_ref.at[pl.ds(0, tile - 2 * piece), :], ga_send.at[k])


def body(rows, cols, lower, rhs, tile_map):
    rhs = rhs[0]
    panels = jnp.transpose(lower[0], (0, 2, 3, 1))
    tiles, tile, width = rhs.shape
    slab = tile // cols
    far = cols // 4
    vmem = pl.BlockSpec(memory_space=pltpu.VMEM)
    dma = pltpu.SemaphoreType.DMA
    lanes = [pltpu.VMEM((cols, slab, width), jnp.bfloat16) for _ in range(6)]
    out = pl.pallas_call(
        functools.partial(kernel, rows, cols),
        name="solve_step",
        out_shape=jax.ShapeDtypeStruct(rhs.shape, jnp.bfloat16),
        in_specs=[pl.BlockSpec(memory_space=pltpu.SMEM), vmem, vmem],
        out_specs=vmem,
        scratch_shapes=[
            *lanes,
            pltpu.VMEM((tiles, tile, width), jnp.bfloat16),
            pltpu.VMEM((tiles, 2, tile, tile), jnp.bfloat16),
            pltpu.VMEM((tile, width), jnp.bfloat16),
            pltpu.VMEM((tile, width), jnp.bfloat16),
            pltpu.VMEM((tiles, tile, width), jnp.float32),
            pltpu.VMEM((tile, tile), jnp.float32),
            pltpu.VMEM((tile // BLOCK, BLOCK, BLOCK), jnp.float32),
            pltpu.VMEM((tile, width), jnp.float32),
            dma((tiles,)), dma((tiles,)), dma((tiles,)), dma((tiles,)),
            dma((far,)), dma((far,)), dma((far,)), dma((far,)),
            dma, dma,
            dma((2,)), dma((2,)), dma((2,)), dma((2,)),
        ],
        compiler_params=pltpu.CompilerParams(
            collective_id=0, has_side_effects=True, vmem_limit_bytes=60 * 1024 * 1024
        ),
    )(tile_map, rhs, panels)
    return out[None]


def solution(mesh):
    rows, cols = mesh.shape["row"], mesh.shape["col"]
    return jax.shard_map(
        functools.partial(body, rows, cols),
        mesh=mesh,
        in_specs=(P("row", None, None, None, "col"), P("row", None, None, "col"), P()),
        out_specs=P("row", None, None, "col"),
        check_vma=False,
    )
```

```python
import functools

import jax
import jax.numpy as jnp
from jax import lax
from jax.experimental import pallas as pl
from jax.experimental.pallas import tpu as pltpu
from jax.sharding import PartitionSpec as P

MESH = pl.DeviceIdType.MESH
BLOCK = 128
VMEM_BYTES = 32 * 1024 * 1024
HIGHEST = lax.Precision.HIGHEST


def dot_f32(a, b):
    return jnp.dot(a, b, preferred_element_type=jnp.float32, precision=HIGHEST)


def halves(a):
    high = a.astype(jnp.bfloat16)
    return high, (a - high.astype(jnp.float32)).astype(jnp.bfloat16)


def dot(a, b):
    return jnp.dot(a, b, preferred_element_type=jnp.float32)


def farthest_first(size):
    return sorted(range(1, size), key=lambda d: -min(d, size - d))


def kernel(
    rows, cols, wide, tm_ref, rhs_ref, lt_ref, out_ref,
    a0, a1, a2, t0, t1, t2, c_ref, g_ref, l_ref, s0_ref, s1_ref, acc_ref, lf_ref, inv_ref, xh_ref, xl_ref,
    p1_send, p1_recv, p2_send, p2_recv, up_send, up_recv, down_send, down_recv,
    pair_send, pair_recv, sc_send, sc_recv, gz_send, gz_recv, gx_send, gx_recv,
):
    a_refs, t_refs = (a0, a1, a2), (t0, t1, t2)
    tiles, tile = rhs_ref.shape[0], rhs_ref.shape[1]
    slab, piece = tile // cols, tile // rows
    chips = cols // 2
    far = chips // 2
    blocks = tile // BLOCK
    row, col = lax.axis_index("row"), lax.axis_index("col")
    chip, core = col // 2, col % 2
    deep = rows // wide
    z, x = row // wide, row % wide

    barrier = pltpu.get_barrier_semaphore()

    def greet_col(d, _):
        pl.semaphore_signal(
            barrier, inc=1, device_id={"col": lax.rem(col + d, cols)}, device_id_type=MESH
        )
        return 0

    def greet_row(d, _):
        pl.semaphore_signal(
            barrier, inc=1, device_id={"row": lax.rem(row + d, rows)}, device_id_type=MESH
        )
        return 0

    lax.fori_loop(1, cols, greet_col, 0)
    lax.fori_loop(1, rows, greet_row, 0)
    g_ref[:, :, pl.ds(pl.multiple_of(col * slab, slab), slab), :] = lt_ref[...]
    pl.semaphore_wait(barrier, cols + rows - 2)

    def at_chip(offset):
        return lax.rem(chip + offset + 2 * chips, chips) * 2 + core

    def rows_of(index, size):
        return pl.ds(pl.multiple_of(index * size, size), size)

    def remote(src, dst, send, recv, target):
        copy = pltpu.make_async_remote_copy(
            src_ref=src, dst_ref=dst, send_sem=send, recv_sem=recv,
            device_id=target, device_id_type=MESH,
        )
        copy.start()

    def drain(ref, sem):
        pltpu.make_async_copy(ref, ref, sem).wait()

    partner = {"col": chip * 2 + 1 - core}

    def panel(ref, part, where, half=None):
        which = 0 if part == 0 else pl.ds(1, tiles - 1)
        if half is None:
            return ref.at[which, :, where, :]
        return ref.at[which, half, where, :]

    def ring_send(part, step, sign):
        half = (0 if sign > 0 else 1) if step == far else None
        block = panel(g_ref, part, rows_of(at_chip(sign * (1 - step)), slab), half)
        src = panel(lt_ref, part, slice(None), half) if step == 1 else block
        send, recv = (up_send, up_recv) if sign > 0 else (down_send, down_recv)
        remote(
            src, block, send.at[part, step - 1], recv.at[part, step - 1], {"col": at_chip(sign)}
        )

    def ring_start(part):
        ring_send(part, 1, 1)
        ring_send(part, 1, -1)
        remote(
            panel(lt_ref, part, slice(None)), panel(g_ref, part, rows_of(col, slab)),
            pair_send.at[part], pair_recv.at[part], partner,
        )

    def ring_block(part, step, sign):
        half = (0 if sign > 0 else 1) if step == far else None
        return panel(g_ref, part, rows_of(at_chip(-sign * step), slab), half)

    def ring_step(part, step):
        for sign, recv in ((1, up_recv), (-1, down_recv)):
            block = ring_block(part, step, sign)
            drain(block, recv.at[part, step - 1])
            if step < far:
                ring_send(part, step + 1, sign)
            remote(block, block, pair_send.at[part], pair_recv.at[part], partner)

    def ring_paired(part, sem):
        drain(panel(g_ref, part, pl.ds(0, tile // 2)), sem.at[part])

    order = []
    for d in range(far, 0, -1):
        order += [d] if d in (far,) else [d, chips - d]
    targets = []
    for d in order:
        targets.append(lax.rem(chip + d, chips) * 2 + core)
        targets.append(lax.rem(chip + d, chips) * 2 + 1 - core)
    targets.append(chip * 2 + 1 - core)

    def phase1(m, some):
        for p in some:
            remote(
                rhs_ref.at[m, rows_of(p, slab), :], a_refs[m].at[col],
                p1_send.at[m], p1_recv.at[m], {"col": p},
            )
        if some is targets or some[-1] is targets[-1]:
            a_refs[m][col] = rhs_ref[m, rows_of(col, slab), :]

    def phase2(m):
        drain(a_refs[m].at[pl.ds(0, cols - 1)], p1_recv.at[m])
        for j in range(cols):
            t_refs[m][j] = a_refs[m][tm_ref[j]]
        c_ref[m, rows_of(col, slab), :] = t_refs[m][col]
        for p in targets:
            remote(
                t_refs[m].at[p], c_ref.at[m, rows_of(col, slab), :],
                p2_send.at[m], p2_recv.at[m], {"col": p},
            )

    def phase2_done(m):
        drain(t_refs[m].at[pl.ds(0, cols - 1)], p2_recv.at[m])

    def invert(k):
        for i in range(blocks):
            for j in range(i + 1):
                u = g_ref[0, k, j * BLOCK : (j + 1) * BLOCK, i * BLOCK : (i + 1) * BLOCK]
                lf_ref[i * BLOCK : (i + 1) * BLOCK, j * BLOCK : (j + 1) * BLOCK] = (
                    u.astype(jnp.float32).T
                )
        r = lax.broadcasted_iota(jnp.int32, (BLOCK, BLOCK), 0)
        c = lax.broadcasted_iota(jnp.int32, (BLOCK, BLOCK), 1)
        eye = r == c
        diag = [
            lf_ref[i * BLOCK : (i + 1) * BLOCK, i * BLOCK : (i + 1) * BLOCK]
            for i in range(blocks)
        ]
        xs = [jnp.where(eye, 1.0 / jnp.where(eye, d, 1.0), 0.0) for d in diag]
        shift = 0
        while (1 << shift) < BLOCK:
            rb, cb = r >> shift, c >> shift
            mask = ((rb >> 1) == (cb >> 1)) & (rb > cb)
            mids = [dot_f32(x, jnp.where(mask, d, 0.0)) for x, d in zip(xs, diag)]
            xs = [x - dot_f32(mid, x) for x, mid in zip(xs, mids)]
            shift += 1
        for i in range(blocks):
            inv_ref[i] = xs[i]

    def solve(work, s_ref):
        for i in range(blocks):
            rng = slice(i * BLOCK, (i + 1) * BLOCK)
            r = work(rng)
            if i:
                left = lf_ref[rng, : i * BLOCK].astype(jnp.bfloat16)
                r = r - (dot(left, xh_ref[: i * BLOCK, :]) + dot(left, xl_ref[: i * BLOCK, :]))
            ih, il = halves(inv_ref[i])
            rh, rl = halves(r)
            sol = dot(ih, rh) + (dot(ih, rl) + dot(il, rh))
            xh_ref[rng, :], xl_ref[rng, :] = halves(sol)
            for g in range(rng.start // piece, rng.stop // piece):
                at = g * piece - rng.start
                s_ref[g // wide, g % wide] = sol[at : at + piece].astype(jnp.bfloat16)

    def put(piece_ref, send, recv, target):
        remote(piece_ref, piece_ref, send, recv, target)

    def scatter(k, s_ref):
        def hops(p):
            dz, dx = abs(p // wide - k // wide), abs(p % wide - k % wide)
            return min(dz, deep - dz) + min(dx, wide - dx)

        for p in sorted((p for p in range(rows) if p != k), key=lambda p: -hops(p)):
            put(s_ref.at[p // wide, p % wide], sc_send.at[k], sc_recv.at[k], {"row": p})

    def gather_z(root, k, s_ref):
        @pl.when(row != root)
        def _():
            drain(s_ref.at[z, x], sc_recv.at[k])

        for d in farthest_first(deep):
            p = lax.rem(z + d, deep) * wide + x

            @pl.when(p != root)
            def _():
                put(s_ref.at[z, x], gz_send.at[k], gz_recv.at[k], {"row": p})

    def gather_x(root, k, s_ref):
        @pl.when(row != root)
        def _():
            drain(s_ref.at[pl.ds(0, deep - 1), 0], gz_recv.at[k])

        for d in farthest_first(wide):
            p = z * wide + lax.rem(x + d, wide)

            @pl.when(p != root)
            def _():
                put(s_ref.at[:, x], gx_send.at[k], gx_recv.at[k], {"row": p})

    def gathered(root, k, s_ref):
        @pl.when(row != root)
        def _():
            drain(s_ref.at[:, pl.ds(0, wide - 1)], gx_recv.at[k])

    def whole(s_ref):
        return s_ref[...].reshape(tile, s_ref.shape[-1])

    def transpose(m):
        for k in range(2):
            for i in range(blocks):
                cut = slice(i * BLOCK, (i + 1) * BLOCK)
                l_ref[m, k, cut, :] = g_ref[m, k, :, cut].T

    def update(m, k, s_ref):
        for i in range(blocks):
            cut = slice(i * BLOCK, (i + 1) * BLOCK)
            term = jnp.dot(l_ref[m, k, cut, :], whole(s_ref), preferred_element_type=jnp.float32)
            if k == 0:
                acc_ref[m, cut, :] = term
            else:
                acc_ref[m, cut, :] = acc_ref[m, cut, :] + term

    scope = jax.named_scope
    quarter = (len(targets) + 3) // 4
    parts = [targets[i * quarter : (i + 1) * quarter] for i in range(4)]
    with scope("start"):
        ring_start(0)
        phase1(0, parts[0])
    for step in range(1, far):
        with scope(f"r0_{step}"):
            ring_step(0, step)
            if parts[step]:
                phase1(0, parts[step])
    for step in range(far, 4):
        if parts[step]:
            phase1(0, parts[step])
    with scope("rr_start"):
        ring_start(1)
    with scope("p2_0"):
        phase2(0)
    with scope("r0_end"):
        ring_step(0, far)
        ring_paired(0, pair_recv)

    @pl.when(row == 0)
    def _():
        with scope("inv0"):
            invert(0)

    @pl.when(row == 1)
    def _():
        with scope("inv1"):
            invert(1)

    with scope("rr1"):
        ring_step(1, 1)
        phase1(1, targets)
    with scope("p2_0_done"):
        phase2_done(0)

    @pl.when(row == 0)
    def _():
        with scope("solve0"):
            solve(lambda rng: c_ref[0, rng, :].astype(jnp.float32), s0_ref)
            scatter(0, s0_ref)

    with scope("tr0"):
        transpose(0)
    with scope("rr2"):
        if far > 2:
            ring_step(1, 2)
        phase1(2, targets)
    with scope("gz0"):
        gather_z(0, 0, s0_ref)
    with scope("gx0"):
        gather_x(0, 0, s0_ref)
    with scope("p2_1"):
        phase2(1)
    with scope("rr3"):
        if far > 3:
            ring_step(1, 3)
    with scope("gx0_done"):
        gathered(0, 0, s0_ref)
    with scope("up00"):
        update(0, 0, s0_ref)

    @pl.when(row == 1)
    def _():
        with scope("solve1"):
            solve(lambda rng: c_ref[0, rng, :].astype(jnp.float32) - acc_ref[0, rng, :], s1_ref)
            scatter(1, s1_ref)

    with scope("gz1"):
        gather_z(1, 1, s1_ref)
    with scope("p2_2"):
        phase2(2)
    with scope("gx1"):
        gather_x(1, 1, s1_ref)
    with scope("rr_end"):
        ring_step(1, far)
    with scope("rr_pair"):
        ring_paired(1, pair_recv)
    with scope("tr12"):
        for m in range(1, tiles):
            transpose(m)
    with scope("up0"):
        for m in range(1, tiles):
            update(m, 0, s0_ref)
    with scope("gx1_done"):
        gathered(1, 1, s1_ref)

    for m in range(tiles):
        with scope(f"up1{m}"):
            update(m, 1, s1_ref)
        with scope(f"fin{m}"):
            if m:
                phase2_done(m)
        with scope(f"out{m}"):
            out_ref[m] = (c_ref[m].astype(jnp.float32) - acc_ref[m]).astype(jnp.bfloat16)

    @pl.when(row == 0)
    def _():
        out_ref[0] = whole(s0_ref)

    @pl.when(row == 1)
    def _():
        out_ref[0] = whole(s1_ref)

    for part in range(2):
        for step in range(1, far + 1):
            drain(ring_block(part, step, 1), up_send.at[part, step - 1])
            drain(ring_block(part, step, -1), down_send.at[part, step - 1])
        ring_paired(part, pair_send)
    for m in range(tiles):
        drain(a_refs[m].at[pl.ds(0, cols - 1)], p1_send.at[m])
        drain(t_refs[m].at[pl.ds(0, cols - 1)], p2_send.at[m])

    def pieces(n):
        return c_ref.at[0, pl.ds(0, n * piece), :]

    for root in range(2):
        near_z = (x == root % wide) & (row != root)
        near_x = (z == root // wide) & (row != root)

        @pl.when(row == root)
        def _():
            drain(pieces(rows - 1), sc_send.at[root])

        for near, sem, count, each in (
            (near_z, gz_send, deep - 1, 1), (near_x, gx_send, wide - 1, deep),
        ):
            if count > 1:
                @pl.when(near)
                def _():
                    drain(pieces((count - 1) * each), sem.at[root])

            @pl.when(jnp.logical_not(near))
            def _():
                drain(pieces(count * each), sem.at[root])


def body(rows, cols, wide, lower, rhs, tile_map):
    rhs = rhs[0]
    panels = jnp.transpose(lower[0], (0, 2, 3, 1))
    tiles, tile, width = rhs.shape
    slab = tile // cols
    far = cols // 4
    vmem = pl.BlockSpec(memory_space=pltpu.VMEM)
    dma = pltpu.SemaphoreType.DMA
    lanes = [pltpu.VMEM((cols, slab, width), jnp.bfloat16) for _ in range(6)]
    out = pl.pallas_call(
        functools.partial(kernel, rows, cols, wide),
        name="solve_step",
        out_shape=jax.ShapeDtypeStruct(rhs.shape, jnp.bfloat16),
        in_specs=[pl.BlockSpec(memory_space=pltpu.SMEM), vmem, vmem],
        out_specs=vmem,
        scratch_shapes=[
            *lanes,
            pltpu.VMEM((tiles, tile, width), jnp.bfloat16),
            pltpu.VMEM((tiles, 2, tile, tile), jnp.bfloat16),
            pltpu.VMEM((tiles, 2, tile, tile), jnp.bfloat16),
            pltpu.VMEM((rows // wide, wide, tile // rows, width), jnp.bfloat16),
            pltpu.VMEM((rows // wide, wide, tile // rows, width), jnp.bfloat16),
            pltpu.VMEM((tiles, tile, width), jnp.float32),
            pltpu.VMEM((tile, tile), jnp.float32),
            pltpu.VMEM((tile // BLOCK, BLOCK, BLOCK), jnp.float32),
            pltpu.VMEM((tile, width), jnp.bfloat16),
            pltpu.VMEM((tile, width), jnp.bfloat16),
            dma((tiles,)), dma((tiles,)), dma((tiles,)), dma((tiles,)),
            dma((2, far)), dma((2, far)), dma((2, far)), dma((2, far)),
            dma((2,)), dma((2,)),
            dma((2,)), dma((2,)), dma((2,)), dma((2,)), dma((2,)), dma((2,)),
        ],
        compiler_params=pltpu.CompilerParams(
            collective_id=0, has_side_effects=True, vmem_limit_bytes=VMEM_BYTES
        ),
    )(tile_map, rhs, panels)
    return out[None]


def solution(mesh):
    rows, cols = mesh.shape["row"], mesh.shape["col"]
    wide = 4 if rows % 16 == 0 else 2
    return jax.shard_map(
        functools.partial(body, rows, cols, wide),
        mesh=mesh,
        in_specs=(P("row", None, None, None, "col"), P("row", None, None, "col"), P()),
        out_specs=P("row", None, None, "col"),
        check_vma=False,
    )
```

```python
import functools

import jax
import jax.numpy as jnp
from jax import lax
from jax.experimental import pallas as pl
from jax.experimental.pallas import tpu as pltpu
from jax.sharding import PartitionSpec as P

MESH = pl.DeviceIdType.MESH
BLOCK = 128
VMEM_BYTES = 54_000_000
HIGHEST = lax.Precision.HIGHEST


def dot_f32(a, b):
    return jnp.dot(a, b, preferred_element_type=jnp.float32, precision=HIGHEST)


def halves(a):
    high = a.astype(jnp.bfloat16)
    return high, (a - high.astype(jnp.float32)).astype(jnp.bfloat16)


def dot(a, b):
    return jnp.dot(a, b, preferred_element_type=jnp.float32)


def farthest_first(size):
    return sorted(range(1, size), key=lambda d: -min(d, size - d))


def kernel(
    rows, cols, wide, tm_hbm, rhs_hbm, lt_hbm, out_ref, tm_ref, rhs_ref, lt_ref,
    a0, a1, a2, t0, t1, t2, c_ref, g_ref, l_ref, s0_ref, s1_ref, acc_ref, lf_ref, inv_ref, xh_ref, xl_ref,
    p1_send, p1_recv, p2_send, p2_recv, up_send, up_recv, down_send, down_recv,
    pair_send, pair_recv, sc_send, sc_recv, gz_send, gz_recv, gx_send, gx_recv, in_sem, ready,
):
    a_refs, t_refs = (a0, a1, a2), (t0, t1, t2)
    tiles, tile = rhs_ref.shape[0], rhs_ref.shape[1]
    slab, piece = tile // cols, tile // rows
    chips = cols // 2
    far = chips // 2
    blocks = tile // BLOCK
    row, col = lax.axis_index("row"), lax.axis_index("col")
    chip, core = col // 2, col % 2
    deep = rows // wide
    z, x = row // wide, row % wide

    load_lt = pltpu.make_async_copy(lt_hbm, lt_ref, in_sem.at[0])
    load_rhs = pltpu.make_async_copy(rhs_hbm, rhs_ref, in_sem.at[1])
    load_tm = pltpu.make_async_copy(tm_hbm, tm_ref, in_sem.at[2])
    for load in (load_lt, load_rhs, load_tm):
        load.start()

    barrier = pltpu.get_barrier_semaphore()

    def greet(target):
        pl.semaphore_signal(barrier, inc=1, device_id=target, device_id_type=MESH)

    for d in farthest_first(cols):
        greet({"col": lax.rem(col + d, cols)})
    for d in farthest_first(deep):
        greet({"row": lax.rem(z + d, deep) * wide + x})
    for d in farthest_first(wide):
        greet({"row": z * wide + lax.rem(x + d, wide)})
    pl.semaphore_wait(barrier, cols + deep + wide - 3)
    for root in range(2):
        @pl.when((x == root) & (z != 0))
        def _():
            pl.semaphore_signal(
                ready.at[root], inc=1, device_id={"row": root}, device_id_type=MESH
            )

    def at_chip(offset):
        return lax.rem(chip + offset + 2 * chips, chips) * 2 + core

    def rows_of(index, size):
        return pl.ds(pl.multiple_of(index * size, size), size)

    def remote(src, dst, send, recv, target):
        copy = pltpu.make_async_remote_copy(
            src_ref=src, dst_ref=dst, send_sem=send, recv_sem=recv,
            device_id=target, device_id_type=MESH,
        )
        copy.start()

    def drain(ref, sem):
        pltpu.make_async_copy(ref, ref, sem).wait()

    partner = {"col": chip * 2 + 1 - core}

    def panel(ref, part, where, half=None):
        which = 0 if part == 0 else pl.ds(1, tiles - 1)
        if half is None:
            return ref.at[which, :, where, :]
        return ref.at[which, half, where, :]

    def ring_send(part, step, sign):
        half = (0 if sign > 0 else 1) if step == far else None
        block = panel(g_ref, part, rows_of(at_chip(sign * (1 - step)), slab), half)
        src = panel(lt_ref, part, slice(None), half) if step == 1 else block
        send, recv = (up_send, up_recv) if sign > 0 else (down_send, down_recv)
        remote(
            src, block, send.at[part, step - 1], recv.at[part, step - 1], {"col": at_chip(sign)}
        )

    def ring_start(part):
        ring_send(part, 1, 1)
        ring_send(part, 1, -1)
        remote(
            panel(lt_ref, part, slice(None)), panel(g_ref, part, rows_of(col, slab)),
            pair_send.at[part], pair_recv.at[part], partner,
        )

    def ring_block(part, step, sign):
        half = (0 if sign > 0 else 1) if step == far else None
        return panel(g_ref, part, rows_of(at_chip(-sign * step), slab), half)

    def ring_step(part, step):
        for sign, recv in ((1, up_recv), (-1, down_recv)):
            block = ring_block(part, step, sign)
            drain(block, recv.at[part, step - 1])
            if step < far:
                ring_send(part, step + 1, sign)
            remote(block, block, pair_send.at[part], pair_recv.at[part], partner)

    def ring_paired(part, sem):
        drain(panel(g_ref, part, pl.ds(0, tile // 2)), sem.at[part])

    order = []
    for d in range(far, 0, -1):
        order += [d] if d in (far,) else [d, chips - d]
    targets = []
    for d in order:
        targets.append(lax.rem(chip + d, chips) * 2 + core)
        targets.append(lax.rem(chip + d, chips) * 2 + 1 - core)
    targets.append(chip * 2 + 1 - core)

    def phase1(m, some):
        for p in some:
            remote(
                rhs_ref.at[m, rows_of(p, slab), :], a_refs[m].at[col],
                p1_send.at[m], p1_recv.at[m], {"col": p},
            )
        if some is targets or some[-1] is targets[-1]:
            a_refs[m][col] = rhs_ref[m, rows_of(col, slab), :]

    def phase2(m):
        drain(a_refs[m].at[pl.ds(0, cols - 1)], p1_recv.at[m])
        for j in range(cols):
            t_refs[m][j] = a_refs[m][tm_ref[j]]
        c_ref[m, rows_of(col, slab), :] = t_refs[m][col]
        for p in targets:
            remote(
                t_refs[m].at[p], c_ref.at[m, rows_of(col, slab), :],
                p2_send.at[m], p2_recv.at[m], {"col": p},
            )

    def phase2_done(m):
        drain(t_refs[m].at[pl.ds(0, cols - 1)], p2_recv.at[m])

    def invert(k):
        for i in range(blocks):
            for j in range(i + 1):
                u = g_ref[0, k, j * BLOCK : (j + 1) * BLOCK, i * BLOCK : (i + 1) * BLOCK]
                lf_ref[i * BLOCK : (i + 1) * BLOCK, j * BLOCK : (j + 1) * BLOCK] = (
                    u.astype(jnp.float32).T
                )
        r = lax.broadcasted_iota(jnp.int32, (BLOCK, BLOCK), 0)
        c = lax.broadcasted_iota(jnp.int32, (BLOCK, BLOCK), 1)
        eye = r == c
        diag = [
            lf_ref[i * BLOCK : (i + 1) * BLOCK, i * BLOCK : (i + 1) * BLOCK]
            for i in range(blocks)
        ]
        xs = [jnp.where(eye, 1.0 / jnp.where(eye, d, 1.0), 0.0) for d in diag]
        shift = 0
        while (1 << shift) < BLOCK:
            rb, cb = r >> shift, c >> shift
            mask = ((rb >> 1) == (cb >> 1)) & (rb > cb)
            mids = [dot_f32(x, jnp.where(mask, d, 0.0)) for x, d in zip(xs, diag)]
            xs = [x - dot_f32(mid, x) for x, mid in zip(xs, mids)]
            shift += 1
        for i in range(blocks):
            inv_ref[i] = xs[i]

    def solve(work, s_ref):
        for i in range(blocks):
            rng = slice(i * BLOCK, (i + 1) * BLOCK)
            r = work(rng)
            if i:
                left = lf_ref[rng, : i * BLOCK].astype(jnp.bfloat16)
                r = r - (dot(left, xh_ref[: i * BLOCK, :]) + dot(left, xl_ref[: i * BLOCK, :]))
            ih, il = halves(inv_ref[i])
            rh, rl = halves(r)
            sol = dot(ih, rh) + (dot(ih, rl) + dot(il, rh))
            xh_ref[rng, :], xl_ref[rng, :] = halves(sol)
            for g in range(rng.start // piece, rng.stop // piece):
                at = g * piece - rng.start
                s_ref[g // wide, g % wide] = sol[at : at + piece].astype(jnp.bfloat16)

    def put(piece_ref, send, recv, target):
        remote(piece_ref, piece_ref, send, recv, target)

    def scatter(k, s_ref):
        pl.semaphore_wait(ready.at[k], deep - 1)

        def hops(p):
            dz, dx = abs(p // wide - k // wide), abs(p % wide - k % wide)
            return min(dz, deep - dz) + min(dx, wide - dx)

        for p in sorted((p for p in range(rows) if p != k), key=lambda p: -hops(p)):
            put(s_ref.at[p // wide, p % wide], sc_send.at[k], sc_recv.at[k], {"row": p})

    def gather_z(root, k, s_ref):
        @pl.when(row != root)
        def _():
            drain(s_ref.at[z, x], sc_recv.at[k])

        for d in farthest_first(deep):
            p = lax.rem(z + d, deep) * wide + x

            @pl.when(p != root)
            def _():
                put(s_ref.at[z, x], gz_send.at[k], gz_recv.at[k], {"row": p})

    def gather_x(root, k, s_ref):
        @pl.when(row != root)
        def _():
            drain(s_ref.at[pl.ds(0, deep - 1), 0], gz_recv.at[k])

        for d in farthest_first(wide):
            p = z * wide + lax.rem(x + d, wide)

            @pl.when(p != root)
            def _():
                put(s_ref.at[:, x], gx_send.at[k], gx_recv.at[k], {"row": p})

    def gathered(root, k, s_ref):
        @pl.when(row != root)
        def _():
            drain(s_ref.at[:, pl.ds(0, wide - 1)], gx_recv.at[k])

    def whole(s_ref):
        return s_ref[...].reshape(tile, s_ref.shape[-1])

    def transpose(m):
        for k in range(2):
            for i in range(blocks):
                cut = slice(i * BLOCK, (i + 1) * BLOCK)
                l_ref[m, k, cut, :] = g_ref[m, k, :, cut].T

    def update(m, k, s_ref):
        for i in range(blocks):
            cut = slice(i * BLOCK, (i + 1) * BLOCK)
            term = jnp.dot(l_ref[m, k, cut, :], whole(s_ref), preferred_element_type=jnp.float32)
            if k == 0:
                acc_ref[m, cut, :] = term
            else:
                acc_ref[m, cut, :] = acc_ref[m, cut, :] + term

    scope = jax.named_scope
    quarter = (len(targets) + 3) // 4
    parts = [targets[i * quarter : (i + 1) * quarter] for i in range(4)]
    with scope("start"):
        load_lt.wait()
        ring_start(0)
        load_rhs.wait()
        phase1(0, parts[0])
        phase1(0, parts[1])
        g_ref[:, :, rows_of(col, slab), :] = lt_ref[...]
    with scope("r0_1"):
        ring_step(0, 1)
        phase1(0, parts[2])
        phase1(0, parts[3])
    if far > 2:
        with scope("r0_2"):
            ring_step(0, 2)
    with scope("rr_start"):
        ring_start(1)
    if far > 3:
        with scope("r0_3"):
            ring_step(0, 3)
    load_tm.wait()
    with scope("p2_0"):
        phase2(0)
    with scope("rr1"):
        ring_step(1, 1)
        phase1(1, targets)
    with scope("r0_end"):
        ring_step(0, far)
        ring_paired(0, pair_recv)

    @pl.when(row == 0)
    def _():
        with scope("inv0"):
            invert(0)

    @pl.when(row == 1)
    def _():
        with scope("inv1"):
            invert(1)

    with scope("p2_0_done"):
        phase2_done(0)

    @pl.when(row == 0)
    def _():
        with scope("solve0"):
            solve(lambda rng: c_ref[0, rng, :].astype(jnp.float32), s0_ref)
            scatter(0, s0_ref)

    with scope("tr0"):
        transpose(0)
    with scope("rr2"):
        if far > 2:
            ring_step(1, 2)
        phase1(2, targets)
    with scope("gz0"):
        gather_z(0, 0, s0_ref)
    with scope("gx0"):
        gather_x(0, 0, s0_ref)
    with scope("p2_1"):
        phase2(1)
    with scope("rr3"):
        if far > 3:
            ring_step(1, 3)
    with scope("gx0_done"):
        gathered(0, 0, s0_ref)
    with scope("up00"):
        update(0, 0, s0_ref)

    @pl.when(row == 1)
    def _():
        with scope("solve1"):
            solve(lambda rng: c_ref[0, rng, :].astype(jnp.float32) - acc_ref[0, rng, :], s1_ref)
            scatter(1, s1_ref)

    with scope("gz1"):
        gather_z(1, 1, s1_ref)
    with scope("p2_2"):
        phase2(2)
    with scope("gx1"):
        gather_x(1, 1, s1_ref)
    with scope("rr_end"):
        ring_step(1, far)
    with scope("rr_pair"):
        ring_paired(1, pair_recv)
    with scope("tr12"):
        for m in range(1, tiles):
            transpose(m)
    with scope("up0"):
        for m in range(1, tiles):
            update(m, 0, s0_ref)
    with scope("gx1_done"):
        gathered(1, 1, s1_ref)

    for m in range(tiles):
        with scope(f"up1{m}"):
            update(m, 1, s1_ref)
        with scope(f"fin{m}"):
            if m:
                phase2_done(m)
        with scope(f"out{m}"):
            out_ref[m] = (c_ref[m].astype(jnp.float32) - acc_ref[m]).astype(jnp.bfloat16)

    @pl.when(row == 0)
    def _():
        out_ref[0] = whole(s0_ref)

    @pl.when(row == 1)
    def _():
        out_ref[0] = whole(s1_ref)

    for part in range(2):
        for step in range(1, far + 1):
            drain(ring_block(part, step, 1), up_send.at[part, step - 1])
            drain(ring_block(part, step, -1), down_send.at[part, step - 1])
        ring_paired(part, pair_send)
    for m in range(tiles):
        drain(a_refs[m].at[pl.ds(0, cols - 1)], p1_send.at[m])
        drain(t_refs[m].at[pl.ds(0, cols - 1)], p2_send.at[m])

    def pieces(n):
        return c_ref.at[0, pl.ds(0, n * piece), :]

    for root in range(2):
        near_z = (x == root % wide) & (row != root)
        near_x = (z == root // wide) & (row != root)

        @pl.when(row == root)
        def _():
            drain(pieces(rows - 1), sc_send.at[root])

        for near, sem, count, each in (
            (near_z, gz_send, deep - 1, 1), (near_x, gx_send, wide - 1, deep),
        ):
            if count > 1:
                @pl.when(near)
                def _():
                    drain(pieces((count - 1) * each), sem.at[root])

            @pl.when(jnp.logical_not(near))
            def _():
                drain(pieces(count * each), sem.at[root])


def body(rows, cols, wide, lower, rhs, tile_map):
    rhs = rhs[0]
    panels = jnp.transpose(lower[0], (0, 2, 3, 1))
    tiles, tile, width = rhs.shape
    slab = tile // cols
    far = cols // 4
    vmem = pl.BlockSpec(memory_space=pltpu.VMEM)
    dma = pltpu.SemaphoreType.DMA
    lanes = [pltpu.VMEM((cols, slab, width), jnp.bfloat16) for _ in range(6)]
    out = pl.pallas_call(
        functools.partial(kernel, rows, cols, wide),
        name="solve_step",
        out_shape=jax.ShapeDtypeStruct(rhs.shape, jnp.bfloat16),
        in_specs=[pl.BlockSpec(memory_space=pl.ANY)] * 3,
        out_specs=vmem,
        scratch_shapes=[
            pltpu.SMEM(tile_map.shape, jnp.int32),
            pltpu.VMEM(rhs.shape, jnp.bfloat16),
            pltpu.VMEM(panels.shape, jnp.bfloat16),
            *lanes,
            pltpu.VMEM((tiles, tile, width), jnp.bfloat16),
            pltpu.VMEM((tiles, 2, tile, tile), jnp.bfloat16),
            pltpu.VMEM((tiles, 2, tile, tile), jnp.bfloat16),
            pltpu.VMEM((rows // wide, wide, tile // rows, width), jnp.bfloat16),
            pltpu.VMEM((rows // wide, wide, tile // rows, width), jnp.bfloat16),
            pltpu.VMEM((tiles, tile, width), jnp.float32),
            pltpu.VMEM((tile, tile), jnp.float32),
            pltpu.VMEM((tile // BLOCK, BLOCK, BLOCK), jnp.float32),
            pltpu.VMEM((tile, width), jnp.bfloat16),
            pltpu.VMEM((tile, width), jnp.bfloat16),
            dma((tiles,)), dma((tiles,)), dma((tiles,)), dma((tiles,)),
            dma((2, far)), dma((2, far)), dma((2, far)), dma((2, far)),
            dma((2,)), dma((2,)),
            dma((2,)), dma((2,)), dma((2,)), dma((2,)), dma((2,)), dma((2,)),
            dma((3,)), pltpu.SemaphoreType.REGULAR((2,)),
        ],
        compiler_params=pltpu.CompilerParams(
            collective_id=0, has_side_effects=True, vmem_limit_bytes=VMEM_BYTES
        ),
    )(tile_map, rhs, panels)
    return out[None]


def solution(mesh):
    rows, cols = mesh.shape["row"], mesh.shape["col"]
    wide = 4 if rows % 16 == 0 else 2
    return jax.shard_map(
        functools.partial(body, rows, cols, wide),
        mesh=mesh,
        in_specs=(P("row", None, None, None, "col"), P("row", None, None, "col"), P()),
        out_specs=P("row", None, None, "col"),
        check_vma=False,
    )
```

```python
import functools

import jax
import jax.numpy as jnp
from jax import lax
from jax.experimental import pallas as pl
from jax.experimental.pallas import tpu as pltpu
from jax.sharding import PartitionSpec as P

MESH = pl.DeviceIdType.MESH
BLOCK = 128
VMEM_BYTES = 58_000_000
HIGHEST = lax.Precision.HIGHEST


def dot_f32(a, b):
    return jnp.dot(a, b, preferred_element_type=jnp.float32, precision=HIGHEST)


def halves(a):
    high = a.astype(jnp.bfloat16)
    return high, (a - high.astype(jnp.float32)).astype(jnp.bfloat16)


def dot(a, b):
    return jnp.dot(a, b, preferred_element_type=jnp.float32)


def farthest_first(size):
    return sorted(range(1, size), key=lambda d: -min(d, size - d))


def kernel(
    rows, cols, wide, tm_hbm, rhs_hbm, lt_hbm, out_ref, tm_ref, rhs_ref, lt_ref,
    a0, a1, a2, t0, t1, t2, c_ref, g_ref, l_ref, s0_ref, s1_ref, acc_ref, lf_ref, inv_ref, xh_ref, xl_ref,
    p1_send, p1_recv, p2_send, p2_recv, up_send, up_recv, down_send, down_recv,
    pair_send, pair_recv, sc_send, sc_recv, gz_send, gz_recv, gx_send, gx_recv, in_sem, ready, seen,
):
    a_refs, t_refs = (a0, a1, a2), (t0, t1, t2)
    tiles, tile = rhs_ref.shape[0], rhs_ref.shape[1]
    slab, piece = tile // cols, tile // rows
    chips = cols // 2
    far = chips // 2
    blocks = tile // BLOCK
    row, col = lax.axis_index("row"), lax.axis_index("col")
    chip, core = col // 2, col % 2
    deep = rows // wide
    z, x = row // wide, row % wide

    load_lt = pltpu.make_async_copy(lt_hbm, lt_ref, in_sem.at[0])
    load_rhs = pltpu.make_async_copy(rhs_hbm, rhs_ref, in_sem.at[1])
    load_tm = pltpu.make_async_copy(tm_hbm, tm_ref, in_sem.at[2])
    for load in (load_lt, load_rhs, load_tm):
        load.start()

    barrier = pltpu.get_barrier_semaphore()

    def signal(sem, **target):
        pl.semaphore_signal(sem, inc=1, device_id=target, device_id_type=MESH)

    def along(sem, sign):
        for d in range(1, deep):
            at = z + sign * d

            @pl.when((at >= 0) & (at < deep))
            def _():
                signal(sem, row=at * wide + x)

        for d in range(1, wide):
            side = x + sign * d

            @pl.when((side >= 0) & (side < wide))
            def _():
                signal(sem, row=z * wide + side)

    for d in farthest_first(cols):
        signal(barrier, col=lax.rem(col + d, cols))
    along(barrier, 1)
    pl.semaphore_wait(barrier, cols - 1 + z + x)
    along(seen, -1)

    def meet():
        higher = deep + wide - 2 - z - x

        @pl.when(higher > 0)
        def _():
            pl.semaphore_wait(seen, higher)

        for root in range(2):
            @pl.when((x == root) & (z != 0))
            def _():
                signal(ready.at[root], row=root)

    def at_chip(offset):
        return lax.rem(chip + offset + 2 * chips, chips) * 2 + core

    def rows_of(index, size):
        return pl.ds(pl.multiple_of(index * size, size), size)

    def remote(src, dst, send, recv, target):
        copy = pltpu.make_async_remote_copy(
            src_ref=src, dst_ref=dst, send_sem=send, recv_sem=recv,
            device_id=target, device_id_type=MESH,
        )
        copy.start()

    def drain(ref, sem):
        pltpu.make_async_copy(ref, ref, sem).wait()

    partner = {"col": chip * 2 + 1 - core}

    def panel(ref, part, where, half=None):
        which = 0 if part == 0 else pl.ds(1, tiles - 1)
        if half is None:
            return ref.at[which, :, where, :]
        return ref.at[which, half, where, :]

    def ring_send(part, step, sign):
        half = (0 if sign > 0 else 1) if step == far else None
        block = panel(g_ref, part, rows_of(at_chip(sign * (1 - step)), slab), half)
        src = panel(lt_ref, part, slice(None), half) if step == 1 else block
        send, recv = (up_send, up_recv) if sign > 0 else (down_send, down_recv)
        remote(
            src, block, send.at[part, step - 1], recv.at[part, step - 1], {"col": at_chip(sign)}
        )

    def ring_start(part):
        ring_send(part, 1, 1)
        ring_send(part, 1, -1)
        remote(
            panel(lt_ref, part, slice(None)), panel(g_ref, part, rows_of(col, slab)),
            pair_send.at[part], pair_recv.at[part], partner,
        )

    def ring_block(part, step, sign):
        half = (0 if sign > 0 else 1) if step == far else None
        return panel(g_ref, part, rows_of(at_chip(-sign * step), slab), half)

    def ring_step(part, step):
        for sign, recv in ((1, up_recv), (-1, down_recv)):
            block = ring_block(part, step, sign)
            drain(block, recv.at[part, step - 1])
            if step < far:
                ring_send(part, step + 1, sign)
            remote(block, block, pair_send.at[part], pair_recv.at[part], partner)

    def ring_paired(part, sem):
        drain(panel(g_ref, part, pl.ds(0, tile // 2)), sem.at[part])

    order = []
    for d in range(far, 0, -1):
        order += [d] if d in (far,) else [d, chips - d]
    targets = []
    for d in order:
        targets.append(lax.rem(chip + d, chips) * 2 + core)
        targets.append(lax.rem(chip + d, chips) * 2 + 1 - core)
    targets.append(chip * 2 + 1 - core)

    def phase1(m, some):
        for p in some:
            remote(
                rhs_ref.at[m, rows_of(p, slab), :], a_refs[m].at[col],
                p1_send.at[m], p1_recv.at[m], {"col": p},
            )
        if some is targets or some[-1] is targets[-1]:
            a_refs[m][col] = rhs_ref[m, rows_of(col, slab), :]

    def phase2(m):
        drain(a_refs[m].at[pl.ds(0, cols - 1)], p1_recv.at[m])
        for j in range(cols):
            t_refs[m][j] = a_refs[m][tm_ref[j]]
        c_ref[m, rows_of(col, slab), :] = t_refs[m][col]
        for p in targets:
            remote(
                t_refs[m].at[p], c_ref.at[m, rows_of(col, slab), :],
                p2_send.at[m], p2_recv.at[m], {"col": p},
            )

    def phase2_done(m):
        drain(t_refs[m].at[pl.ds(0, cols - 1)], p2_recv.at[m])

    def invert(k):
        for i in range(blocks):
            for j in range(i + 1):
                u = g_ref[0, k, j * BLOCK : (j + 1) * BLOCK, i * BLOCK : (i + 1) * BLOCK]
                lf_ref[i * BLOCK : (i + 1) * BLOCK, j * BLOCK : (j + 1) * BLOCK] = (
                    u.astype(jnp.float32).T
                )
        r = lax.broadcasted_iota(jnp.int32, (BLOCK, BLOCK), 0)
        c = lax.broadcasted_iota(jnp.int32, (BLOCK, BLOCK), 1)
        eye = r == c
        diag = [
            lf_ref[i * BLOCK : (i + 1) * BLOCK, i * BLOCK : (i + 1) * BLOCK]
            for i in range(blocks)
        ]
        xs = [jnp.where(eye, 1.0 / jnp.where(eye, d, 1.0), 0.0) for d in diag]
        shift = 0
        while (1 << shift) < BLOCK:
            rb, cb = r >> shift, c >> shift
            mask = ((rb >> 1) == (cb >> 1)) & (rb > cb)
            mids = [dot_f32(x, jnp.where(mask, d, 0.0)) for x, d in zip(xs, diag)]
            xs = [x - dot_f32(mid, x) for x, mid in zip(xs, mids)]
            shift += 1
        for i in range(blocks):
            inv_ref[i] = xs[i]

    def solve(work, s_ref):
        for i in range(blocks):
            rng = slice(i * BLOCK, (i + 1) * BLOCK)
            r = work(rng)
            if i:
                left = lf_ref[rng, : i * BLOCK].astype(jnp.bfloat16)
                r = r - (dot(left, xh_ref[: i * BLOCK, :]) + dot(left, xl_ref[: i * BLOCK, :]))
            ih, il = halves(inv_ref[i])
            rh, rl = halves(r)
            sol = dot(ih, rh) + (dot(ih, rl) + dot(il, rh))
            xh_ref[rng, :], xl_ref[rng, :] = halves(sol)
            for g in range(rng.start // piece, rng.stop // piece):
                at = g * piece - rng.start
                s_ref[g // wide, g % wide] = sol[at : at + piece].astype(jnp.bfloat16)

    def put(piece_ref, send, recv, target):
        remote(piece_ref, piece_ref, send, recv, target)

    def scatter(k, s_ref):
        pl.semaphore_wait(ready.at[k], deep - 1)

        def hops(p):
            dz, dx = abs(p // wide - k // wide), abs(p % wide - k % wide)
            return min(dz, deep - dz) + min(dx, wide - dx)

        for p in sorted((p for p in range(rows) if p != k), key=lambda p: -hops(p)):
            put(s_ref.at[p // wide, p % wide], sc_send.at[k], sc_recv.at[k], {"row": p})

    def gather_z(root, k, s_ref):
        @pl.when(row != root)
        def _():
            drain(s_ref.at[z, x], sc_recv.at[k])

        for d in farthest_first(deep):
            p = lax.rem(z + d, deep) * wide + x

            @pl.when(p != root)
            def _():
                put(s_ref.at[z, x], gz_send.at[k], gz_recv.at[k], {"row": p})

    def gather_x(root, k, s_ref):
        @pl.when(row != root)
        def _():
            drain(s_ref.at[pl.ds(0, deep - 1), 0], gz_recv.at[k])

        for d in farthest_first(wide):
            p = z * wide + lax.rem(x + d, wide)

            @pl.when(p != root)
            def _():
                put(s_ref.at[:, x], gx_send.at[k], gx_recv.at[k], {"row": p})

    def gathered(root, k, s_ref):
        @pl.when(row != root)
        def _():
            drain(s_ref.at[:, pl.ds(0, wide - 1)], gx_recv.at[k])

    def whole(s_ref):
        return s_ref[...].reshape(tile, s_ref.shape[-1])

    def transpose(m):
        for k in range(2):
            for i in range(blocks):
                cut = slice(i * BLOCK, (i + 1) * BLOCK)
                l_ref[m, k, cut, :] = g_ref[m, k, :, cut].T

    def update(m, k, s_ref):
        for i in range(blocks):
            cut = slice(i * BLOCK, (i + 1) * BLOCK)
            term = jnp.dot(l_ref[m, k, cut, :], whole(s_ref), preferred_element_type=jnp.float32)
            if k == 0:
                acc_ref[m, cut, :] = term
            else:
                acc_ref[m, cut, :] = acc_ref[m, cut, :] + term

    scope = jax.named_scope
    quarter = (len(targets) + 3) // 4
    parts = [targets[i * quarter : (i + 1) * quarter] for i in range(4)]
    with scope("start"):
        load_lt.wait()
        ring_start(0)
        load_rhs.wait()
        phase1(0, parts[0])
        phase1(0, parts[1])
        g_ref[:, :, rows_of(col, slab), :] = lt_ref[...]
    with scope("r0_1"):
        ring_step(0, 1)
        phase1(0, parts[2])
        phase1(0, parts[3])
    if far > 2:
        with scope("r0_2"):
            ring_step(0, 2)
    with scope("rr_start"):
        ring_start(1)
    with scope("meet"):
        meet()
    if far > 3:
        with scope("r0_3"):
            ring_step(0, 3)
    load_tm.wait()
    with scope("p2_0"):
        phase2(0)
    with scope("rr1"):
        ring_step(1, 1)
        phase1(1, targets)
    with scope("r0_end"):
        ring_step(0, far)
        ring_paired(0, pair_recv)

    @pl.when(row == 0)
    def _():
        with scope("inv0"):
            invert(0)

    @pl.when(row == 1)
    def _():
        with scope("inv1"):
            invert(1)

    with scope("p2_0_done"):
        phase2_done(0)

    @pl.when(row == 0)
    def _():
        with scope("solve0"):
            solve(lambda rng: c_ref[0, rng, :].astype(jnp.float32), s0_ref)
            scatter(0, s0_ref)

    with scope("tr0"):
        transpose(0)
    with scope("rr2"):
        if far > 2:
            ring_step(1, 2)
        phase1(2, targets)
    with scope("gz0"):
        gather_z(0, 0, s0_ref)
    with scope("gx0"):
        gather_x(0, 0, s0_ref)
    with scope("p2_1"):
        phase2(1)
    with scope("rr3"):
        if far > 3:
            ring_step(1, 3)
    with scope("gx0_done"):
        gathered(0, 0, s0_ref)
    with scope("up00"):
        update(0, 0, s0_ref)

    @pl.when(row == 1)
    def _():
        with scope("solve1"):
            solve(lambda rng: c_ref[0, rng, :].astype(jnp.float32) - acc_ref[0, rng, :], s1_ref)
            scatter(1, s1_ref)

    with scope("gz1"):
        gather_z(1, 1, s1_ref)
    with scope("p2_2"):
        phase2(2)
    with scope("gx1"):
        gather_x(1, 1, s1_ref)
    with scope("rr_end"):
        ring_step(1, far)
    with scope("rr_pair"):
        ring_paired(1, pair_recv)
    with scope("tr12"):
        for m in range(1, tiles):
            transpose(m)
    with scope("up0"):
        for m in range(1, tiles):
            update(m, 0, s0_ref)
    with scope("gx1_done"):
        gathered(1, 1, s1_ref)

    for m in range(tiles):
        with scope(f"up1{m}"):
            update(m, 1, s1_ref)
        with scope(f"fin{m}"):
            if m:
                phase2_done(m)
        with scope(f"out{m}"):
            out_ref[m] = (c_ref[m].astype(jnp.float32) - acc_ref[m]).astype(jnp.bfloat16)

    @pl.when(row == 0)
    def _():
        out_ref[0] = whole(s0_ref)

    @pl.when(row == 1)
    def _():
        out_ref[0] = whole(s1_ref)

    for part in range(2):
        for step in range(1, far + 1):
            drain(ring_block(part, step, 1), up_send.at[part, step - 1])
            drain(ring_block(part, step, -1), down_send.at[part, step - 1])
        ring_paired(part, pair_send)
    for m in range(tiles):
        drain(a_refs[m].at[pl.ds(0, cols - 1)], p1_send.at[m])
        drain(t_refs[m].at[pl.ds(0, cols - 1)], p2_send.at[m])

    def pieces(n):
        return c_ref.at[0, pl.ds(0, n * piece), :]

    for root in range(2):
        near_z = (x == root % wide) & (row != root)
        near_x = (z == root // wide) & (row != root)

        @pl.when(row == root)
        def _():
            drain(pieces(rows - 1), sc_send.at[root])

        for near, sem, count, each in (
            (near_z, gz_send, deep - 1, 1), (near_x, gx_send, wide - 1, deep),
        ):
            if count > 1:
                @pl.when(near)
                def _():
                    drain(pieces((count - 1) * each), sem.at[root])

            @pl.when(jnp.logical_not(near))
            def _():
                drain(pieces(count * each), sem.at[root])


def body(rows, cols, wide, lower, rhs, tile_map):
    rhs = rhs[0]
    panels = jnp.transpose(lower[0], (0, 2, 3, 1))
    tiles, tile, width = rhs.shape
    slab = tile // cols
    far = cols // 4
    vmem = pl.BlockSpec(memory_space=pltpu.VMEM)
    dma = pltpu.SemaphoreType.DMA
    lanes = [pltpu.VMEM((cols, slab, width), jnp.bfloat16) for _ in range(6)]
    out = pl.pallas_call(
        functools.partial(kernel, rows, cols, wide),
        name="solve_step",
        out_shape=pltpu.VMEM(rhs.shape, jnp.bfloat16),
        in_specs=[pl.BlockSpec(memory_space=pl.ANY)] * 3,
        out_specs=vmem,
        scratch_shapes=[
            pltpu.SMEM(tile_map.shape, jnp.int32),
            pltpu.VMEM(rhs.shape, jnp.bfloat16),
            pltpu.VMEM(panels.shape, jnp.bfloat16),
            *lanes,
            pltpu.VMEM((tiles, tile, width), jnp.bfloat16),
            pltpu.VMEM((tiles, 2, tile, tile), jnp.bfloat16),
            pltpu.VMEM((tiles, 2, tile, tile), jnp.bfloat16),
            pltpu.VMEM((rows // wide, wide, tile // rows, width), jnp.bfloat16),
            pltpu.VMEM((rows // wide, wide, tile // rows, width), jnp.bfloat16),
            pltpu.VMEM((tiles, tile, width), jnp.float32),
            pltpu.VMEM((tile, tile), jnp.float32),
            pltpu.VMEM((tile // BLOCK, BLOCK, BLOCK), jnp.float32),
            pltpu.VMEM((tile, width), jnp.bfloat16),
            pltpu.VMEM((tile, width), jnp.bfloat16),
            dma((tiles,)), dma((tiles,)), dma((tiles,)), dma((tiles,)),
            dma((2, far)), dma((2, far)), dma((2, far)), dma((2, far)),
            dma((2,)), dma((2,)),
            dma((2,)), dma((2,)), dma((2,)), dma((2,)), dma((2,)), dma((2,)),
            dma((3,)), pltpu.SemaphoreType.REGULAR((2,)),
            pltpu.SemaphoreType.REGULAR,
        ],
        compiler_params=pltpu.CompilerParams(
            collective_id=0, has_side_effects=True, vmem_limit_bytes=VMEM_BYTES
        ),
    )(tile_map, rhs, panels)
    return out[None]


def solution(mesh):
    rows, cols = mesh.shape["row"], mesh.shape["col"]
    wide = 4 if rows % 16 == 0 else 2
    return jax.shard_map(
        functools.partial(body, rows, cols, wide),
        mesh=mesh,
        in_specs=(P("row", None, None, None, "col"), P("row", None, None, "col"), P()),
        out_specs=P("row", None, None, "col"),
        check_vma=False,
    )
```

```python
import functools

import jax
import jax.numpy as jnp
from jax import lax
from jax.experimental import pallas as pl
from jax.experimental.pallas import tpu as pltpu
from jax.sharding import PartitionSpec as P

MESH = pl.DeviceIdType.MESH
BLOCK = 128
VMEM_BYTES = 58_000_000
HIGHEST = lax.Precision.HIGHEST


def dot_f32(a, b):
    return jnp.dot(a, b, preferred_element_type=jnp.float32, precision=HIGHEST)


def halves(a):
    high = a.astype(jnp.bfloat16)
    return high, (a - high.astype(jnp.float32)).astype(jnp.bfloat16)


def dot(a, b):
    return jnp.dot(a, b, preferred_element_type=jnp.float32)


def farthest_first(size):
    return sorted(range(1, size), key=lambda d: -min(d, size - d))


def kernel(
    rows, cols, wide, tm_hbm, rhs_hbm, lt_hbm, out_ref, tm_ref, rhs_ref, lt_ref,
    a0, a1, a2, t0, t1, t2, c_ref, g_ref, l_ref, s0_ref, s1_ref, acc_ref, lf_ref, inv_ref, xh_ref, xl_ref,
    p1_send, p1_recv, p2_send, p2_recv, up_send, up_recv, down_send, down_recv,
    pair_send, pair_recv, sc_send, sc_recv, gz_send, gz_recv, gx_send, gx_recv, in_sem, ready, seen, late,
):
    a_refs, t_refs = (a0, a1, a2), (t0, t1, t2)
    tiles, tile = rhs_ref.shape[0], rhs_ref.shape[1]
    slab, piece = tile // cols, tile // rows
    chips = cols // 2
    far = chips // 2
    blocks = tile // BLOCK
    row, col = lax.axis_index("row"), lax.axis_index("col")
    chip, core = col // 2, col % 2
    deep = rows // wide
    z, x = row // wide, row % wide

    load_lt = pltpu.make_async_copy(lt_hbm, lt_ref, in_sem.at[0])
    load_rhs = pltpu.make_async_copy(rhs_hbm.at[0], rhs_ref.at[0], in_sem.at[1])
    load_rest = pltpu.make_async_copy(
        rhs_hbm.at[pl.ds(1, tiles - 1)], rhs_ref.at[pl.ds(1, tiles - 1)], in_sem.at[3]
    )
    load_tm = pltpu.make_async_copy(tm_hbm, tm_ref, in_sem.at[2])
    load_lt.start()
    load_rhs.start()

    barrier = pltpu.get_barrier_semaphore()

    def signal(sem, **target):
        pl.semaphore_signal(sem, inc=1, device_id=target, device_id_type=MESH)

    def along(sem, sign):
        for d in range(1, deep):
            at = z + sign * d

            @pl.when((at >= 0) & (at < deep))
            def _():
                signal(sem, row=at * wide + x)

        for d in range(1, wide):
            side = x + sign * d

            @pl.when((side >= 0) & (side < wide))
            def _():
                signal(sem, row=z * wide + side)

    tardy = row == 0

    @pl.when(jnp.logical_not(tardy & (col == 0)))
    def _():
        for d in farthest_first(cols):
            signal(barrier, col=lax.rem(col + d, cols))

    along(barrier, 1)
    load_rest.start()
    load_tm.start()
    pl.semaphore_wait(barrier, jnp.where(tardy & (col != 0), cols - 2, cols - 1) + z + x)

    @pl.when(tardy & (col == 0))
    def _():
        for d in farthest_first(cols):
            signal(late, col=d)


    def meet():
        higher = deep + wide - 2 - z - x

        @pl.when(higher > 0)
        def _():
            pl.semaphore_wait(seen, higher)

        for root in range(2):
            @pl.when((x == root) & (z != 0))
            def _():
                signal(ready.at[root], row=root)

    def at_chip(offset):
        return lax.rem(chip + offset + 2 * chips, chips) * 2 + core

    def rows_of(index, size):
        return pl.ds(pl.multiple_of(index * size, size), size)

    def remote(src, dst, send, recv, target):
        copy = pltpu.make_async_remote_copy(
            src_ref=src, dst_ref=dst, send_sem=send, recv_sem=recv,
            device_id=target, device_id_type=MESH,
        )
        copy.start()

    def drain(ref, sem):
        pltpu.make_async_copy(ref, ref, sem).wait()

    partner = {"col": chip * 2 + 1 - core}

    def panel(ref, part, where, half=None):
        which = 0 if part == 0 else pl.ds(1, tiles - 1)
        if half is None:
            return ref.at[which, :, where, :]
        return ref.at[which, half, where, :]

    def ring_send(part, step, sign):
        half = (0 if sign > 0 else 1) if step == far else None
        block = panel(g_ref, part, rows_of(at_chip(sign * (1 - step)), slab), half)
        src = panel(lt_ref, part, slice(None), half) if step == 1 else block
        send, recv = (up_send, up_recv) if sign > 0 else (down_send, down_recv)
        remote(
            src, block, send.at[part, step - 1], recv.at[part, step - 1], {"col": at_chip(sign)}
        )

    def ring_start(part, waited=None):
        def send(target, act):
            if waited is None:
                act()
            elif waited:
                pl.when(tardy & (target == 0))(act)
            else:
                pl.when(jnp.logical_not(tardy & (target == 0)))(act)

        send(at_chip(1), lambda: ring_send(part, 1, 1))
        send(at_chip(-1), lambda: ring_send(part, 1, -1))
        send(
            chip * 2 + 1 - core,
            lambda: remote(
                panel(lt_ref, part, slice(None)), panel(g_ref, part, rows_of(col, slab)),
                pair_send.at[part], pair_recv.at[part], partner,
            ),
        )

    def ring_block(part, step, sign):
        half = (0 if sign > 0 else 1) if step == far else None
        return panel(g_ref, part, rows_of(at_chip(-sign * step), slab), half)

    def ring_step(part, step):
        for sign, recv in ((1, up_recv), (-1, down_recv)):
            block = ring_block(part, step, sign)
            drain(block, recv.at[part, step - 1])
            if step < far:
                ring_send(part, step + 1, sign)
            remote(block, block, pair_send.at[part], pair_recv.at[part], partner)

    def ring_paired(part, sem):
        drain(panel(g_ref, part, pl.ds(0, tile // 2)), sem.at[part])

    order = []
    for d in range(far, 0, -1):
        order += [d] if d in (far,) else [d, chips - d]
    targets = []
    for d in order:
        targets.append(lax.rem(chip + d, chips) * 2 + core)
        targets.append(lax.rem(chip + d, chips) * 2 + 1 - core)
    targets.append(chip * 2 + 1 - core)

    def hop1(m, p):
        remote(
            rhs_ref.at[m, rows_of(p, slab), :], a_refs[m].at[col],
            p1_send.at[m], p1_recv.at[m], {"col": p},
        )

    def phase1(m, some):
        for p in some:
            if m:
                hop1(m, p)
            else:
                pl.when(jnp.logical_not(tardy & (p == 0)))(functools.partial(hop1, m, p))
        if some[-1] is targets[-1]:
            a_refs[m][col] = rhs_ref[m, rows_of(col, slab), :]

    def phase2(m):
        drain(a_refs[m].at[pl.ds(0, cols - 1)], p1_recv.at[m])
        for j in range(cols):
            t_refs[m][j] = a_refs[m][tm_ref[j]]
        c_ref[m, rows_of(col, slab), :] = t_refs[m][col]
        for p in targets:
            remote(
                t_refs[m].at[p], c_ref.at[m, rows_of(col, slab), :],
                p2_send.at[m], p2_recv.at[m], {"col": p},
            )

    def phase2_done(m):
        drain(t_refs[m].at[pl.ds(0, cols - 1)], p2_recv.at[m])

    def invert(k):
        for i in range(blocks):
            for j in range(i + 1):
                u = g_ref[0, k, j * BLOCK : (j + 1) * BLOCK, i * BLOCK : (i + 1) * BLOCK]
                lf_ref[i * BLOCK : (i + 1) * BLOCK, j * BLOCK : (j + 1) * BLOCK] = (
                    u.astype(jnp.float32).T
                )
        r = lax.broadcasted_iota(jnp.int32, (BLOCK, BLOCK), 0)
        c = lax.broadcasted_iota(jnp.int32, (BLOCK, BLOCK), 1)
        eye = r == c
        diag = [
            lf_ref[i * BLOCK : (i + 1) * BLOCK, i * BLOCK : (i + 1) * BLOCK]
            for i in range(blocks)
        ]
        xs = [jnp.where(eye, 1.0 / jnp.where(eye, d, 1.0), 0.0) for d in diag]
        shift = 0
        while (1 << shift) < BLOCK:
            rb, cb = r >> shift, c >> shift
            mask = ((rb >> 1) == (cb >> 1)) & (rb > cb)
            mids = [dot_f32(x, jnp.where(mask, d, 0.0)) for x, d in zip(xs, diag)]
            xs = [x - dot_f32(mid, x) for x, mid in zip(xs, mids)]
            shift += 1
        for i in range(blocks):
            inv_ref[i] = xs[i]

    def solve(work, s_ref):
        for i in range(blocks):
            rng = slice(i * BLOCK, (i + 1) * BLOCK)
            r = work(rng)
            if i:
                left = lf_ref[rng, : i * BLOCK].astype(jnp.bfloat16)
                r = r - (dot(left, xh_ref[: i * BLOCK, :]) + dot(left, xl_ref[: i * BLOCK, :]))
            ih, il = halves(inv_ref[i])
            rh, rl = halves(r)
            sol = dot(ih, rh) + (dot(ih, rl) + dot(il, rh))
            xh_ref[rng, :], xl_ref[rng, :] = halves(sol)
            for g in range(rng.start // piece, rng.stop // piece):
                at = g * piece - rng.start
                s_ref[g // wide, g % wide] = sol[at : at + piece].astype(jnp.bfloat16)

    def put(piece_ref, send, recv, target):
        remote(piece_ref, piece_ref, send, recv, target)

    def scatter(k, s_ref):
        pl.semaphore_wait(ready.at[k], deep - 1)

        def hops(p):
            dz, dx = abs(p // wide - k // wide), abs(p % wide - k % wide)
            return min(dz, deep - dz) + min(dx, wide - dx)

        for p in sorted((p for p in range(rows) if p != k), key=lambda p: -hops(p)):
            put(s_ref.at[p // wide, p % wide], sc_send.at[k], sc_recv.at[k], {"row": p})

    def gather_z(root, k, s_ref):
        @pl.when(row != root)
        def _():
            drain(s_ref.at[z, x], sc_recv.at[k])

        for d in farthest_first(deep):
            p = lax.rem(z + d, deep) * wide + x

            @pl.when(p != root)
            def _():
                put(s_ref.at[z, x], gz_send.at[k], gz_recv.at[k], {"row": p})

    def gather_x(root, k, s_ref):
        @pl.when(row != root)
        def _():
            drain(s_ref.at[pl.ds(0, deep - 1), 0], gz_recv.at[k])

        for d in farthest_first(wide):
            p = z * wide + lax.rem(x + d, wide)

            @pl.when(p != root)
            def _():
                put(s_ref.at[:, x], gx_send.at[k], gx_recv.at[k], {"row": p})

    def gathered(root, k, s_ref):
        @pl.when(row != root)
        def _():
            drain(s_ref.at[:, pl.ds(0, wide - 1)], gx_recv.at[k])

    def whole(s_ref):
        return s_ref[...].reshape(tile, s_ref.shape[-1])

    def transpose(m):
        for k in range(2):
            for i in range(blocks):
                cut = slice(i * BLOCK, (i + 1) * BLOCK)
                l_ref[m, k, cut, :] = g_ref[m, k, :, cut].T

    def update(m, k, s_ref):
        for i in range(blocks):
            cut = slice(i * BLOCK, (i + 1) * BLOCK)
            term = jnp.dot(l_ref[m, k, cut, :], whole(s_ref), preferred_element_type=jnp.float32)
            if k == 0:
                acc_ref[m, cut, :] = term
            else:
                acc_ref[m, cut, :] = acc_ref[m, cut, :] + term

    scope = jax.named_scope
    quarter = (len(targets) + 3) // 4
    parts = [targets[i * quarter : (i + 1) * quarter] for i in range(4)]
    with scope("start"):
        load_lt.wait()
        ring_start(0, False)
        load_rhs.wait()
        phase1(0, parts[0])

        @pl.when(tardy & (col != 0))
        def _():
            pl.semaphore_wait(late, 1)
            hop1(0, 0)

        ring_start(0, True)
        phase1(0, parts[1])
        along(seen, -1)
        g_ref[:, :, rows_of(col, slab), :] = lt_ref[...]
    with scope("r0_1"):
        ring_step(0, 1)
        phase1(0, parts[2])
        phase1(0, parts[3])
    if far > 2:
        with scope("r0_2"):
            ring_step(0, 2)
    with scope("rr_start"):
        ring_start(1)
    with scope("meet"):
        meet()
    if far > 3:
        with scope("r0_3"):
            ring_step(0, 3)
    load_tm.wait()
    with scope("p2_0"):
        phase2(0)
    load_rest.wait()
    with scope("rr1"):
        ring_step(1, 1)
        phase1(1, targets)
    with scope("r0_end"):
        ring_step(0, far)
        ring_paired(0, pair_recv)

    @pl.when(row == 0)
    def _():
        with scope("inv0"):
            invert(0)

    @pl.when(row == 1)
    def _():
        with scope("inv1"):
            invert(1)

    with scope("p2_0_done"):
        phase2_done(0)

    @pl.when(row == 0)
    def _():
        with scope("solve0"):
            solve(lambda rng: c_ref[0, rng, :].astype(jnp.float32), s0_ref)
            scatter(0, s0_ref)

    with scope("tr0"):
        transpose(0)
    with scope("rr2"):
        if far > 2:
            ring_step(1, 2)
        phase1(2, targets)
    with scope("gz0"):
        gather_z(0, 0, s0_ref)
    with scope("gx0"):
        gather_x(0, 0, s0_ref)
    with scope("p2_1"):
        phase2(1)
    with scope("rr3"):
        if far > 3:
            ring_step(1, 3)
    with scope("gx0_done"):
        gathered(0, 0, s0_ref)
    with scope("up00"):
        update(0, 0, s0_ref)

    @pl.when(row == 1)
    def _():
        with scope("solve1"):
            solve(lambda rng: c_ref[0, rng, :].astype(jnp.float32) - acc_ref[0, rng, :], s1_ref)
            scatter(1, s1_ref)

    with scope("gz1"):
        gather_z(1, 1, s1_ref)
    with scope("p2_2"):
        phase2(2)
    with scope("gx1"):
        gather_x(1, 1, s1_ref)
    with scope("rr_end"):
        ring_step(1, far)
    with scope("rr_pair"):
        ring_paired(1, pair_recv)
    with scope("tr12"):
        for m in range(1, tiles):
            transpose(m)
    with scope("up0"):
        for m in range(1, tiles):
            update(m, 0, s0_ref)
    with scope("gx1_done"):
        gathered(1, 1, s1_ref)

    for m in range(tiles):
        with scope(f"up1{m}"):
            update(m, 1, s1_ref)
        with scope(f"fin{m}"):
            if m:
                phase2_done(m)
        with scope(f"out{m}"):
            out_ref[m] = (c_ref[m].astype(jnp.float32) - acc_ref[m]).astype(jnp.bfloat16)

    @pl.when(row == 0)
    def _():
        out_ref[0] = whole(s0_ref)

    @pl.when(row == 1)
    def _():
        out_ref[0] = whole(s1_ref)

    for part in range(2):
        for step in range(1, far + 1):
            drain(ring_block(part, step, 1), up_send.at[part, step - 1])
            drain(ring_block(part, step, -1), down_send.at[part, step - 1])
        ring_paired(part, pair_send)
    for m in range(tiles):
        drain(a_refs[m].at[pl.ds(0, cols - 1)], p1_send.at[m])
        drain(t_refs[m].at[pl.ds(0, cols - 1)], p2_send.at[m])

    def pieces(n):
        return c_ref.at[0, pl.ds(0, n * piece), :]

    for root in range(2):
        near_z = (x == root % wide) & (row != root)
        near_x = (z == root // wide) & (row != root)

        @pl.when(row == root)
        def _():
            drain(pieces(rows - 1), sc_send.at[root])

        for near, sem, count, each in (
            (near_z, gz_send, deep - 1, 1), (near_x, gx_send, wide - 1, deep),
        ):
            if count > 1:
                @pl.when(near)
                def _():
                    drain(pieces((count - 1) * each), sem.at[root])

            @pl.when(jnp.logical_not(near))
            def _():
                drain(pieces(count * each), sem.at[root])


def body(rows, cols, wide, lower, rhs, tile_map):
    rhs = rhs[0]
    panels = jnp.transpose(lower[0], (0, 2, 3, 1))
    tiles, tile, width = rhs.shape
    slab = tile // cols
    far = cols // 4
    vmem = pl.BlockSpec(memory_space=pltpu.VMEM)
    dma = pltpu.SemaphoreType.DMA
    lanes = [pltpu.VMEM((cols, slab, width), jnp.bfloat16) for _ in range(6)]
    out = pl.pallas_call(
        functools.partial(kernel, rows, cols, wide),
        name="solve_step",
        out_shape=pltpu.VMEM(rhs.shape, jnp.bfloat16),
        in_specs=[pl.BlockSpec(memory_space=pl.ANY)] * 3,
        out_specs=vmem,
        scratch_shapes=[
            pltpu.SMEM(tile_map.shape, jnp.int32),
            pltpu.VMEM(rhs.shape, jnp.bfloat16),
            pltpu.VMEM(panels.shape, jnp.bfloat16),
            *lanes,
            pltpu.VMEM((tiles, tile, width), jnp.bfloat16),
            pltpu.VMEM((tiles, 2, tile, tile), jnp.bfloat16),
            pltpu.VMEM((tiles, 2, tile, tile), jnp.bfloat16),
            pltpu.VMEM((rows // wide, wide, tile // rows, width), jnp.bfloat16),
            pltpu.VMEM((rows // wide, wide, tile // rows, width), jnp.bfloat16),
            pltpu.VMEM((tiles, tile, width), jnp.float32),
            pltpu.VMEM((tile, tile), jnp.float32),
            pltpu.VMEM((tile // BLOCK, BLOCK, BLOCK), jnp.float32),
            pltpu.VMEM((tile, width), jnp.bfloat16),
            pltpu.VMEM((tile, width), jnp.bfloat16),
            dma((tiles,)), dma((tiles,)), dma((tiles,)), dma((tiles,)),
            dma((2, far)), dma((2, far)), dma((2, far)), dma((2, far)),
            dma((2,)), dma((2,)),
            dma((2,)), dma((2,)), dma((2,)), dma((2,)), dma((2,)), dma((2,)),
            dma((4,)), pltpu.SemaphoreType.REGULAR((2,)),
            pltpu.SemaphoreType.REGULAR, pltpu.SemaphoreType.REGULAR,
        ],
        compiler_params=pltpu.CompilerParams(
            collective_id=0, has_side_effects=True, vmem_limit_bytes=VMEM_BYTES
        ),
    )(tile_map, rhs, panels)
    return out[None]


def solution(mesh):
    rows, cols = mesh.shape["row"], mesh.shape["col"]
    wide = 4 if rows % 16 == 0 else 2
    return jax.shard_map(
        functools.partial(body, rows, cols, wide),
        mesh=mesh,
        in_specs=(P("row", None, None, None, "col"), P("row", None, None, "col"), P()),
        out_specs=P("row", None, None, "col"),
        check_vma=False,
    )
```

```python
import functools

import jax
import jax.numpy as jnp
from jax import lax
from jax.experimental import pallas as pl
from jax.experimental.pallas import tpu as pltpu
from jax.sharding import PartitionSpec as P

MESH = pl.DeviceIdType.MESH
BLOCK = 128
VMEM_BYTES = 58_000_000
HIGHEST = lax.Precision.HIGHEST


def dot_f32(a, b):
    return jnp.dot(a, b, preferred_element_type=jnp.float32, precision=HIGHEST)


def farthest_first(size):
    return sorted(range(1, size), key=lambda d: -min(d, size - d))


def kernel(
    rows, cols, wide, tm_hbm, rhs_hbm, lt_hbm, out_ref, tm_ref, rhs_ref, lt_ref,
    a0, a1, a2, t0, t1, t2, c_ref, g_ref, l_ref, s0_ref, s1_ref, acc_ref, lf_ref, inv_ref, x_ref,
    p1_send, p1_recv, p2_send, p2_recv, up_send, up_recv, down_send, down_recv,
    pair_send, pair_recv, sc_send, sc_recv, gz_send, gz_recv, gx_send, gx_recv, in_sem, ready, seen, late,
):
    a_refs, t_refs = (a0, a1, a2), (t0, t1, t2)
    tiles, tile = rhs_ref.shape[0], rhs_ref.shape[1]
    slab, piece = tile // cols, tile // rows
    chips = cols // 2
    far = chips // 2
    blocks = tile // BLOCK
    row, col = lax.axis_index("row"), lax.axis_index("col")
    chip, core = col // 2, col % 2
    deep = rows // wide
    z, x = row // wide, row % wide

    load_lt = pltpu.make_async_copy(lt_hbm, lt_ref, in_sem.at[0])
    load_rhs = pltpu.make_async_copy(rhs_hbm.at[0], rhs_ref.at[0], in_sem.at[1])
    load_rest = pltpu.make_async_copy(
        rhs_hbm.at[pl.ds(1, tiles - 1)], rhs_ref.at[pl.ds(1, tiles - 1)], in_sem.at[3]
    )
    load_tm = pltpu.make_async_copy(tm_hbm, tm_ref, in_sem.at[2])
    load_lt.start()
    load_rhs.start()

    barrier = pltpu.get_barrier_semaphore()

    def signal(sem, **target):
        pl.semaphore_signal(sem, inc=1, device_id=target, device_id_type=MESH)

    def along(sem, sign):
        for d in range(1, deep):
            at = z + sign * d

            @pl.when((at >= 0) & (at < deep))
            def _():
                signal(sem, row=at * wide + x)

        for d in range(1, wide):
            side = x + sign * d

            @pl.when((side >= 0) & (side < wide))
            def _():
                signal(sem, row=z * wide + side)

    tardy = row == 0

    @pl.when(jnp.logical_not(tardy & (col == 0)))
    def _():
        for d in farthest_first(cols):
            signal(barrier, col=lax.rem(col + d, cols))

    along(barrier, 1)
    load_rest.start()
    load_tm.start()
    pl.semaphore_wait(barrier, jnp.where(tardy & (col != 0), cols - 2, cols - 1) + z + x)

    @pl.when(tardy & (col == 0))
    def _():
        for d in farthest_first(cols):
            signal(late, col=d)


    def meet():
        higher = deep + wide - 2 - z - x

        @pl.when(higher > 0)
        def _():
            pl.semaphore_wait(seen, higher)

        for root in range(2):
            @pl.when((x == root) & (z != 0))
            def _():
                signal(ready.at[root], row=root)

    def at_chip(offset):
        return lax.rem(chip + offset + 2 * chips, chips) * 2 + core

    def rows_of(index, size):
        return pl.ds(pl.multiple_of(index * size, size), size)

    def remote(src, dst, send, recv, target):
        copy = pltpu.make_async_remote_copy(
            src_ref=src, dst_ref=dst, send_sem=send, recv_sem=recv,
            device_id=target, device_id_type=MESH,
        )
        copy.start()

    def drain(ref, sem):
        pltpu.make_async_copy(ref, ref, sem).wait()

    partner = {"col": chip * 2 + 1 - core}

    def panel(ref, part, where, half=None):
        which = 0 if part == 0 else pl.ds(1, tiles - 1)
        if half is None:
            return ref.at[which, :, where, :]
        return ref.at[which, half, where, :]

    def ring_send(part, step, sign):
        half = (0 if sign > 0 else 1) if step == far else None
        block = panel(g_ref, part, rows_of(at_chip(sign * (1 - step)), slab), half)
        src = panel(lt_ref, part, slice(None), half) if step == 1 else block
        send, recv = (up_send, up_recv) if sign > 0 else (down_send, down_recv)
        remote(
            src, block, send.at[part, step - 1], recv.at[part, step - 1], {"col": at_chip(sign)}
        )

    def ring_start(part, waited=None):
        def send(target, act):
            if waited is None:
                act()
            elif waited:
                pl.when(tardy & (target == 0))(act)
            else:
                pl.when(jnp.logical_not(tardy & (target == 0)))(act)

        send(at_chip(1), lambda: ring_send(part, 1, 1))
        send(at_chip(-1), lambda: ring_send(part, 1, -1))
        send(
            chip * 2 + 1 - core,
            lambda: remote(
                panel(lt_ref, part, slice(None)), panel(g_ref, part, rows_of(col, slab)),
                pair_send.at[part], pair_recv.at[part], partner,
            ),
        )

    def ring_block(part, step, sign):
        half = (0 if sign > 0 else 1) if step == far else None
        return panel(g_ref, part, rows_of(at_chip(-sign * step), slab), half)

    def ring_step(part, step):
        for sign, recv in ((1, up_recv), (-1, down_recv)):
            block = ring_block(part, step, sign)
            drain(block, recv.at[part, step - 1])
            if step < far:
                ring_send(part, step + 1, sign)
            remote(block, block, pair_send.at[part], pair_recv.at[part], partner)

    def ring_paired(part, sem):
        drain(panel(g_ref, part, pl.ds(0, tile // 2)), sem.at[part])

    order = []
    for d in range(far, 0, -1):
        order += [d] if d in (far,) else [d, chips - d]
    targets = []
    for d in order:
        targets.append(lax.rem(chip + d, chips) * 2 + core)
        targets.append(lax.rem(chip + d, chips) * 2 + 1 - core)
    targets.append(chip * 2 + 1 - core)

    def hop1(m, p):
        remote(
            rhs_ref.at[m, rows_of(p, slab), :], a_refs[m].at[col],
            p1_send.at[m], p1_recv.at[m], {"col": p},
        )

    def phase1(m, some):
        for p in some:
            if m:
                hop1(m, p)
            else:
                pl.when(jnp.logical_not(tardy & (p == 0)))(functools.partial(hop1, m, p))
        if some[-1] is targets[-1]:
            a_refs[m][col] = rhs_ref[m, rows_of(col, slab), :]

    def phase2(m):
        drain(a_refs[m].at[pl.ds(0, cols - 1)], p1_recv.at[m])
        for j in range(cols):
            t_refs[m][j] = a_refs[m][tm_ref[j]]
        c_ref[m, rows_of(col, slab), :] = t_refs[m][col]
        for p in targets:
            remote(
                t_refs[m].at[p], c_ref.at[m, rows_of(col, slab), :],
                p2_send.at[m], p2_recv.at[m], {"col": p},
            )

    def phase2_done(m):
        drain(t_refs[m].at[pl.ds(0, cols - 1)], p2_recv.at[m])

    def invert(k):
        for i in range(blocks):
            for j in range(i + 1):
                u = g_ref[0, k, j * BLOCK : (j + 1) * BLOCK, i * BLOCK : (i + 1) * BLOCK]
                lf_ref[i * BLOCK : (i + 1) * BLOCK, j * BLOCK : (j + 1) * BLOCK] = (
                    u.astype(jnp.float32).T
                )
        r = lax.broadcasted_iota(jnp.int32, (BLOCK, BLOCK), 0)
        c = lax.broadcasted_iota(jnp.int32, (BLOCK, BLOCK), 1)
        eye = r == c
        diag = [
            lf_ref[i * BLOCK : (i + 1) * BLOCK, i * BLOCK : (i + 1) * BLOCK]
            for i in range(blocks)
        ]
        xs = [jnp.where(eye, 1.0 / jnp.where(eye, d, 1.0), 0.0) for d in diag]
        shift = 0
        while (1 << shift) < BLOCK:
            rb, cb = r >> shift, c >> shift
            mask = ((rb >> 1) == (cb >> 1)) & (rb > cb)
            mids = [dot_f32(x, jnp.where(mask, d, 0.0)) for x, d in zip(xs, diag)]
            xs = [x - dot_f32(mid, x) for x, mid in zip(xs, mids)]
            shift += 1
        for i in range(blocks):
            inv_ref[i] = xs[i]

    def solve(work, s_ref):
        for i in range(blocks):
            rng = slice(i * BLOCK, (i + 1) * BLOCK)
            r = work(rng)
            if i:
                r = r - dot_f32(lf_ref[rng, : i * BLOCK], x_ref[: i * BLOCK, :])
            sol = dot_f32(inv_ref[i], r)
            x_ref[rng, :] = sol
            for g in range(rng.start // piece, rng.stop // piece):
                at = g * piece - rng.start
                s_ref[g // wide, g % wide] = sol[at : at + piece].astype(jnp.bfloat16)

    def put(piece_ref, send, recv, target):
        remote(piece_ref, piece_ref, send, recv, target)

    def scatter(k, s_ref):
        pl.semaphore_wait(ready.at[k], deep - 1)

        def hops(p):
            dz, dx = abs(p // wide - k // wide), abs(p % wide - k % wide)
            return min(dz, deep - dz) + min(dx, wide - dx)

        for p in sorted((p for p in range(rows) if p != k), key=lambda p: -hops(p)):
            put(s_ref.at[p // wide, p % wide], sc_send.at[k], sc_recv.at[k], {"row": p})

    def gather_z(root, k, s_ref):
        @pl.when(row != root)
        def _():
            drain(s_ref.at[z, x], sc_recv.at[k])

        for d in farthest_first(deep):
            p = lax.rem(z + d, deep) * wide + x

            @pl.when(p != root)
            def _():
                put(s_ref.at[z, x], gz_send.at[k], gz_recv.at[k], {"row": p})

    def gather_x(root, k, s_ref):
        @pl.when(row != root)
        def _():
            drain(s_ref.at[pl.ds(0, deep - 1), 0], gz_recv.at[k])

        for d in farthest_first(wide):
            p = z * wide + lax.rem(x + d, wide)

            @pl.when(p != root)
            def _():
                put(s_ref.at[:, x], gx_send.at[k], gx_recv.at[k], {"row": p})

    def gathered(root, k, s_ref):
        @pl.when(row != root)
        def _():
            drain(s_ref.at[:, pl.ds(0, wide - 1)], gx_recv.at[k])

    def whole(s_ref):
        return s_ref[...].reshape(tile, s_ref.shape[-1])

    def transpose(m):
        for k in range(2):
            for i in range(blocks):
                cut = slice(i * BLOCK, (i + 1) * BLOCK)
                l_ref[m, k, cut, :] = g_ref[m, k, :, cut].T

    def update(m, k, s_ref):
        for i in range(blocks):
            cut = slice(i * BLOCK, (i + 1) * BLOCK)
            term = jnp.dot(l_ref[m, k, cut, :], whole(s_ref), preferred_element_type=jnp.float32)
            if k == 0:
                acc_ref[m, cut, :] = term
            else:
                acc_ref[m, cut, :] = acc_ref[m, cut, :] + term

    scope = jax.named_scope
    quarter = (len(targets) + 3) // 4
    parts = [targets[i * quarter : (i + 1) * quarter] for i in range(4)]
    with scope("start"):
        load_lt.wait()
        ring_start(0, False)
        load_rhs.wait()
        phase1(0, parts[0])

        @pl.when(tardy & (col != 0))
        def _():
            pl.semaphore_wait(late, 1)
            hop1(0, 0)

        ring_start(0, True)
        phase1(0, parts[1])
        along(seen, -1)
        g_ref[:, :, rows_of(col, slab), :] = lt_ref[...]
    with scope("r0_1"):
        ring_step(0, 1)
        phase1(0, parts[2])
        phase1(0, parts[3])
    if far > 2:
        with scope("r0_2"):
            ring_step(0, 2)
    with scope("rr_start"):
        ring_start(1)
    with scope("meet"):
        meet()
    if far > 3:
        with scope("r0_3"):
            ring_step(0, 3)
    load_tm.wait()
    with scope("p2_0"):
        phase2(0)
    load_rest.wait()
    with scope("rr1"):
        ring_step(1, 1)
        phase1(1, targets)
    with scope("r0_end"):
        ring_step(0, far)
        ring_paired(0, pair_recv)

    @pl.when(row == 0)
    def _():
        with scope("inv0"):
            invert(0)

    @pl.when(row == 1)
    def _():
        with scope("inv1"):
            invert(1)

    with scope("p2_0_done"):
        phase2_done(0)

    @pl.when(row == 0)
    def _():
        with scope("solve0"):
            solve(lambda rng: c_ref[0, rng, :].astype(jnp.float32), s0_ref)
            scatter(0, s0_ref)

    with scope("tr0"):
        transpose(0)
    with scope("rr2"):
        if far > 2:
            ring_step(1, 2)
        phase1(2, targets)
    with scope("gz0"):
        gather_z(0, 0, s0_ref)
    with scope("gx0"):
        gather_x(0, 0, s0_ref)
    with scope("p2_1"):
        phase2(1)
    with scope("rr3"):
        if far > 3:
            ring_step(1, 3)
    with scope("gx0_done"):
        gathered(0, 0, s0_ref)
    with scope("up00"):
        update(0, 0, s0_ref)

    @pl.when(row == 1)
    def _():
        with scope("solve1"):
            solve(lambda rng: c_ref[0, rng, :].astype(jnp.float32) - acc_ref[0, rng, :], s1_ref)
            scatter(1, s1_ref)

    with scope("gz1"):
        gather_z(1, 1, s1_ref)
    with scope("p2_2"):
        phase2(2)
    with scope("gx1"):
        gather_x(1, 1, s1_ref)
    with scope("rr_end"):
        ring_step(1, far)
    with scope("rr_pair"):
        ring_paired(1, pair_recv)
    with scope("tr12"):
        for m in range(1, tiles):
            transpose(m)
    with scope("up0"):
        for m in range(1, tiles):
            update(m, 0, s0_ref)
    with scope("gx1_done"):
        gathered(1, 1, s1_ref)

    for m in range(tiles):
        with scope(f"up1{m}"):
            update(m, 1, s1_ref)
        with scope(f"fin{m}"):
            if m:
                phase2_done(m)
        with scope(f"out{m}"):
            out_ref[m] = (c_ref[m].astype(jnp.float32) - acc_ref[m]).astype(jnp.bfloat16)

    @pl.when(row == 0)
    def _():
        out_ref[0] = whole(s0_ref)

    @pl.when(row == 1)
    def _():
        out_ref[0] = whole(s1_ref)

    for part in range(2):
        for step in range(1, far + 1):
            drain(ring_block(part, step, 1), up_send.at[part, step - 1])
            drain(ring_block(part, step, -1), down_send.at[part, step - 1])
        ring_paired(part, pair_send)
    for m in range(tiles):
        drain(a_refs[m].at[pl.ds(0, cols - 1)], p1_send.at[m])
        drain(t_refs[m].at[pl.ds(0, cols - 1)], p2_send.at[m])

    def pieces(n):
        return c_ref.at[0, pl.ds(0, n * piece), :]

    for root in range(2):
        near_z = (x == root % wide) & (row != root)
        near_x = (z == root // wide) & (row != root)

        @pl.when(row == root)
        def _():
            drain(pieces(rows - 1), sc_send.at[root])

        for near, sem, count, each in (
            (near_z, gz_send, deep - 1, 1), (near_x, gx_send, wide - 1, deep),
        ):
            if count > 1:
                @pl.when(near)
                def _():
                    drain(pieces((count - 1) * each), sem.at[root])

            @pl.when(jnp.logical_not(near))
            def _():
                drain(pieces(count * each), sem.at[root])


def body(rows, cols, wide, lower, rhs, tile_map):
    rhs = rhs[0]
    panels = jnp.transpose(lower[0], (0, 2, 3, 1))
    tiles, tile, width = rhs.shape
    slab = tile // cols
    far = cols // 4
    vmem = pl.BlockSpec(memory_space=pltpu.VMEM)
    dma = pltpu.SemaphoreType.DMA
    lanes = [pltpu.VMEM((cols, slab, width), jnp.bfloat16) for _ in range(6)]
    out = pl.pallas_call(
        functools.partial(kernel, rows, cols, wide),
        name="solve_step",
        out_shape=pltpu.VMEM(rhs.shape, jnp.bfloat16),
        in_specs=[pl.BlockSpec(memory_space=pl.ANY)] * 3,
        out_specs=vmem,
        scratch_shapes=[
            pltpu.SMEM(tile_map.shape, jnp.int32),
            pltpu.VMEM(rhs.shape, jnp.bfloat16),
            pltpu.VMEM(panels.shape, jnp.bfloat16),
            *lanes,
            pltpu.VMEM((tiles, tile, width), jnp.bfloat16),
            pltpu.VMEM((tiles, 2, tile, tile), jnp.bfloat16),
            pltpu.VMEM((tiles, 2, tile, tile), jnp.bfloat16),
            pltpu.VMEM((rows // wide, wide, tile // rows, width), jnp.bfloat16),
            pltpu.VMEM((rows // wide, wide, tile // rows, width), jnp.bfloat16),
            pltpu.VMEM((tiles, tile, width), jnp.float32),
            pltpu.VMEM((tile, tile), jnp.float32),
            pltpu.VMEM((tile // BLOCK, BLOCK, BLOCK), jnp.float32),
            pltpu.VMEM((tile, width), jnp.float32),
            dma((tiles,)), dma((tiles,)), dma((tiles,)), dma((tiles,)),
            dma((2, far)), dma((2, far)), dma((2, far)), dma((2, far)),
            dma((2,)), dma((2,)),
            dma((2,)), dma((2,)), dma((2,)), dma((2,)), dma((2,)), dma((2,)),
            dma((4,)), pltpu.SemaphoreType.REGULAR((2,)),
            pltpu.SemaphoreType.REGULAR, pltpu.SemaphoreType.REGULAR,
        ],
        compiler_params=pltpu.CompilerParams(
            collective_id=0, has_side_effects=True, vmem_limit_bytes=VMEM_BYTES
        ),
    )(tile_map, rhs, panels)
    return out[None]


def solution(mesh):
    rows, cols = mesh.shape["row"], mesh.shape["col"]
    wide = 4 if rows % 16 == 0 else 2
    return jax.shard_map(
        functools.partial(body, rows, cols, wide),
        mesh=mesh,
        in_specs=(P("row", None, None, None, "col"), P("row", None, None, "col"), P()),
        out_specs=P("row", None, None, "col"),
        check_vma=False,
    )
```

```python
import functools

import jax
import jax.numpy as jnp
from jax import lax
from jax.experimental import pallas as pl
from jax.experimental.pallas import tpu as pltpu
from jax.sharding import PartitionSpec as P

MESH = pl.DeviceIdType.MESH
BLOCK = 128
VMEM_BYTES = 58_000_000
HIGHEST = lax.Precision.HIGHEST


def dot_f32(a, b):
    return jnp.dot(a, b, preferred_element_type=jnp.float32, precision=HIGHEST)


def farthest_first(size):
    return sorted(range(1, size), key=lambda d: -min(d, size - d))


def kernel(
    rows, cols, wide, tm_hbm, rhs_hbm, lt_hbm, out_ref, tm_ref, rhs_ref, lt_ref,
    a0, a1, a2, t0, t1, t2, c_ref, g_ref, l_ref, s0_ref, s1_ref, acc_ref, lf_ref, inv_ref, x_ref,
    p1_send, p1_recv, p2_send, p2_recv, up_send, up_recv, down_send, down_recv,
    pair_send, pair_recv, sc_send, sc_recv, gz_send, gz_recv, gx_send, gx_recv, in_sem, ready, seen, late,
):
    a_refs, t_refs = (a0, a1, a2), (t0, t1, t2)
    tiles, tile = rhs_ref.shape[0], rhs_ref.shape[1]
    slab, piece = tile // cols, tile // rows
    chips = cols // 2
    far = chips // 2
    blocks = tile // BLOCK
    row, col = lax.axis_index("row"), lax.axis_index("col")
    chip, core = col // 2, col % 2
    deep = rows // wide
    z, x = row // wide, row % wide

    load_lt = pltpu.make_async_copy(lt_hbm, lt_ref, in_sem.at[0])
    load_rhs = pltpu.make_async_copy(rhs_hbm.at[0], rhs_ref.at[0], in_sem.at[1])
    load_rest = pltpu.make_async_copy(
        rhs_hbm.at[pl.ds(1, tiles - 1)], rhs_ref.at[pl.ds(1, tiles - 1)], in_sem.at[3]
    )
    load_tm = pltpu.make_async_copy(tm_hbm, tm_ref, in_sem.at[2])
    load_lt.start()
    load_rhs.start()

    barrier = pltpu.get_barrier_semaphore()

    def signal(sem, **target):
        pl.semaphore_signal(sem, inc=1, device_id=target, device_id_type=MESH)

    def along(sem, sign):
        for d in range(1, deep):
            at = z + sign * d

            @pl.when((at >= 0) & (at < deep))
            def _():
                signal(sem, row=at * wide + x)

        for d in range(1, wide):
            side = x + sign * d

            @pl.when((side >= 0) & (side < wide))
            def _():
                signal(sem, row=z * wide + side)

    tardy = row == 0

    @pl.when(jnp.logical_not(tardy & (col == 0)))
    def _():
        for d in farthest_first(cols):
            signal(barrier, col=lax.rem(col + d, cols))

    along(barrier, 1)
    load_rest.start()
    load_tm.start()
    pl.semaphore_wait(barrier, jnp.where(tardy & (col != 0), cols - 2, cols - 1) + z + x)

    @pl.when(tardy & (col == 0))
    def _():
        for d in farthest_first(cols):
            signal(late, col=d)


    def meet():
        higher = deep + wide - 2 - z - x

        @pl.when(higher > 0)
        def _():
            pl.semaphore_wait(seen, higher)

        for root in range(2):
            @pl.when((x == root) & (z != 0))
            def _():
                signal(ready.at[root], row=root)

    def at_chip(offset):
        return lax.rem(chip + offset + 2 * chips, chips) * 2 + core

    def rows_of(index, size):
        return pl.ds(pl.multiple_of(index * size, size), size)

    def remote(src, dst, send, recv, target):
        copy = pltpu.make_async_remote_copy(
            src_ref=src, dst_ref=dst, send_sem=send, recv_sem=recv,
            device_id=target, device_id_type=MESH,
        )
        copy.start()

    def drain(ref, sem):
        pltpu.make_async_copy(ref, ref, sem).wait()

    partner = {"col": chip * 2 + 1 - core}

    def panel(ref, part, where, half=None):
        which = 0 if part == 0 else pl.ds(1, tiles - 1)
        if half is None:
            return ref.at[which, :, where, :]
        return ref.at[which, half, where, :]

    def ring_send(part, step, sign):
        half = (0 if sign > 0 else 1) if step == far else None
        block = panel(g_ref, part, rows_of(at_chip(sign * (1 - step)), slab), half)
        src = panel(lt_ref, part, slice(None), half) if step == 1 else block
        send, recv = (up_send, up_recv) if sign > 0 else (down_send, down_recv)
        remote(
            src, block, send.at[part, step - 1], recv.at[part, step - 1], {"col": at_chip(sign)}
        )

    def ring_start(part, waited=None):
        def send(target, act):
            if waited is None:
                act()
            elif waited:
                pl.when(tardy & (target == 0))(act)
            else:
                pl.when(jnp.logical_not(tardy & (target == 0)))(act)

        send(at_chip(1), lambda: ring_send(part, 1, 1))
        send(at_chip(-1), lambda: ring_send(part, 1, -1))
        send(
            chip * 2 + 1 - core,
            lambda: remote(
                panel(lt_ref, part, slice(None)), panel(g_ref, part, rows_of(col, slab)),
                pair_send.at[part], pair_recv.at[part], partner,
            ),
        )

    def ring_block(part, step, sign):
        half = (0 if sign > 0 else 1) if step == far else None
        return panel(g_ref, part, rows_of(at_chip(-sign * step), slab), half)

    def ring_step(part, step):
        for sign, recv in ((1, up_recv), (-1, down_recv)):
            block = ring_block(part, step, sign)
            drain(block, recv.at[part, step - 1])
            if step < far:
                ring_send(part, step + 1, sign)
            remote(block, block, pair_send.at[part], pair_recv.at[part], partner)

    def ring_paired(part, sem):
        drain(panel(g_ref, part, pl.ds(0, tile // 2)), sem.at[part])

    order = []
    for d in range(far, 0, -1):
        order += [d] if d in (far,) else [d, chips - d]
    targets = []
    for d in order:
        targets.append(lax.rem(chip + d, chips) * 2 + core)
        targets.append(lax.rem(chip + d, chips) * 2 + 1 - core)
    targets.append(chip * 2 + 1 - core)

    def hop1(m, p):
        remote(
            rhs_ref.at[m, rows_of(p, slab), :], a_refs[m].at[col],
            p1_send.at[m], p1_recv.at[m], {"col": p},
        )

    def phase1(m, some):
        for p in some:
            if m:
                hop1(m, p)
            else:
                pl.when(jnp.logical_not(tardy & (p == 0)))(functools.partial(hop1, m, p))
        if some[-1] is targets[-1]:
            a_refs[m][col] = rhs_ref[m, rows_of(col, slab), :]

    def phase2(m):
        drain(a_refs[m].at[pl.ds(0, cols - 1)], p1_recv.at[m])
        for j in range(cols):
            t_refs[m][j] = a_refs[m][tm_ref[j]]
        c_ref[m, rows_of(col, slab), :] = t_refs[m][col]
        for p in targets:
            remote(
                t_refs[m].at[p], c_ref.at[m, rows_of(col, slab), :],
                p2_send.at[m], p2_recv.at[m], {"col": p},
            )

    def phase2_done(m):
        drain(t_refs[m].at[pl.ds(0, cols - 1)], p2_recv.at[m])

    def invert(k):
        for i in range(blocks):
            for j in range(i + 1):
                u = g_ref[0, k, j * BLOCK : (j + 1) * BLOCK, i * BLOCK : (i + 1) * BLOCK]
                lf_ref[i * BLOCK : (i + 1) * BLOCK, j * BLOCK : (j + 1) * BLOCK] = (
                    u.astype(jnp.float32).T
                )
        r = lax.broadcasted_iota(jnp.int32, (BLOCK, BLOCK), 0)
        c = lax.broadcasted_iota(jnp.int32, (BLOCK, BLOCK), 1)
        eye = r == c
        diag = [
            lf_ref[i * BLOCK : (i + 1) * BLOCK, i * BLOCK : (i + 1) * BLOCK]
            for i in range(blocks)
        ]
        xs = [jnp.where(eye, 1.0 / jnp.where(eye, d, 1.0), 0.0) for d in diag]
        shift = 0
        while (1 << shift) < BLOCK:
            rb, cb = r >> shift, c >> shift
            mask = ((rb >> 1) == (cb >> 1)) & (rb > cb)
            mids = [dot_f32(x, jnp.where(mask, d, 0.0)) for x, d in zip(xs, diag)]
            xs = [x - dot_f32(mid, x) for x, mid in zip(xs, mids)]
            shift += 1
        for i in range(blocks):
            inv_ref[i] = xs[i]

    def solve(work, s_ref):
        for i in range(blocks):
            rng = slice(i * BLOCK, (i + 1) * BLOCK)
            r = work(rng)
            if i:
                r = r - dot_f32(lf_ref[rng, : i * BLOCK], x_ref[: i * BLOCK, :])
            sol = dot_f32(inv_ref[i], r)
            x_ref[rng, :] = sol
            for g in range(rng.start // piece, rng.stop // piece):
                at = g * piece - rng.start
                s_ref[g // wide, g % wide] = sol[at : at + piece].astype(jnp.bfloat16)

    def put(piece_ref, send, recv, target):
        remote(piece_ref, piece_ref, send, recv, target)

    def scatter(k, s_ref):
        pl.semaphore_wait(ready.at[k], deep - 1)

        def hops(p):
            dz, dx = abs(p // wide - k // wide), abs(p % wide - k % wide)
            return min(dz, deep - dz) + min(dx, wide - dx)

        for p in sorted((p for p in range(rows) if p != k), key=lambda p: -hops(p)):
            put(s_ref.at[p // wide, p % wide], sc_send.at[k], sc_recv.at[k], {"row": p})

    def gather_z(root, k, s_ref):
        @pl.when(row != root)
        def _():
            drain(s_ref.at[z, x], sc_recv.at[k])

        for d in farthest_first(deep):
            p = lax.rem(z + d, deep) * wide + x

            @pl.when(p != root)
            def _():
                put(s_ref.at[z, x], gz_send.at[k], gz_recv.at[k], {"row": p})

    def gather_x(root, k, s_ref):
        @pl.when(row != root)
        def _():
            drain(s_ref.at[pl.ds(0, deep - 1), 0], gz_recv.at[k])

        for d in farthest_first(wide):
            p = z * wide + lax.rem(x + d, wide)

            @pl.when(p != root)
            def _():
                put(s_ref.at[:, x], gx_send.at[k], gx_recv.at[k], {"row": p})

    def gathered(root, k, s_ref):
        @pl.when(row != root)
        def _():
            drain(s_ref.at[:, pl.ds(0, wide - 1)], gx_recv.at[k])

    def whole(s_ref):
        return s_ref[...].reshape(tile, s_ref.shape[-1])

    def transpose(m):
        for k in range(2):
            for i in range(blocks):
                cut = slice(i * BLOCK, (i + 1) * BLOCK)
                l_ref[m, k, cut, :] = g_ref[m, k, :, cut].T

    def update(m, k, s_ref):
        for i in range(blocks):
            cut = slice(i * BLOCK, (i + 1) * BLOCK)
            term = jnp.dot(l_ref[m, k, cut, :], whole(s_ref), preferred_element_type=jnp.float32)
            if k == 0:
                acc_ref[m, cut, :] = term
            else:
                acc_ref[m, cut, :] = acc_ref[m, cut, :] + term

    scope = jax.named_scope
    quarter = (len(targets) + 3) // 4
    parts = [targets[i * quarter : (i + 1) * quarter] for i in range(4)]
    with scope("start"):
        load_lt.wait()
        ring_start(0, False)
        load_rhs.wait()
        phase1(0, parts[0])

        @pl.when(tardy & (col != 0))
        def _():
            pl.semaphore_wait(late, 1)
            hop1(0, 0)

        ring_start(0, True)
        phase1(0, parts[1])
        along(seen, -1)
        g_ref[:, :, rows_of(col, slab), :] = lt_ref[...]
    with scope("r0_1"):
        ring_step(0, 1)
        phase1(0, parts[2])
        phase1(0, parts[3])
    if far > 2:
        with scope("r0_2"):
            ring_step(0, 2)
    with scope("rr_start"):
        ring_start(1)
    with scope("meet"):
        meet()
    if far > 3:
        with scope("r0_3"):
            ring_step(0, 3)
    load_tm.wait()
    with scope("p2_0"):
        phase2(0)
    load_rest.wait()
    with scope("rr1"):
        ring_step(1, 1)
        phase1(1, targets)
    with scope("r0_end"):
        ring_step(0, far)
        ring_paired(0, pair_recv)

    @pl.when(row == 0)
    def _():
        with scope("inv0"):
            invert(0)

    @pl.when(row == 1)
    def _():
        with scope("inv1"):
            invert(1)

    with scope("p2_0_done"):
        phase2_done(0)

    @pl.when(row == 0)
    def _():
        with scope("solve0"):
            solve(lambda rng: c_ref[0, rng, :].astype(jnp.float32), s0_ref)
            scatter(0, s0_ref)

    with scope("tr0"):
        transpose(0)
    with scope("rr2"):
        if far > 2:
            ring_step(1, 2)
        phase1(2, targets)
    with scope("gz0"):
        gather_z(0, 0, s0_ref)
    with scope("gx0"):
        gather_x(0, 0, s0_ref)
    with scope("p2_1"):
        phase2(1)
    with scope("rr3"):
        if far > 3:
            ring_step(1, 3)
    with scope("gx0_done"):
        gathered(0, 0, s0_ref)
    with scope("up00"):
        update(0, 0, s0_ref)

    @pl.when(row == 1)
    def _():
        with scope("solve1"):
            solve(lambda rng: c_ref[0, rng, :].astype(jnp.float32) - acc_ref[0, rng, :], s1_ref)
            scatter(1, s1_ref)

    with scope("gz1"):
        gather_z(1, 1, s1_ref)
    with scope("p2_2"):
        phase2(2)
    with scope("gx1"):
        gather_x(1, 1, s1_ref)
    with scope("rr_end"):
        ring_step(1, far)
    with scope("rr_pair"):
        ring_paired(1, pair_recv)
    with scope("tr12"):
        for m in range(1, tiles):
            transpose(m)
    with scope("up0"):
        for m in range(1, tiles):
            update(m, 0, s0_ref)
    with scope("gx1_done"):
        gathered(1, 1, s1_ref)

    for m in range(tiles):
        with scope(f"up1{m}"):
            update(m, 1, s1_ref)

    def finish(m):
        out_ref[m] = (c_ref[m].astype(jnp.float32) - acc_ref[m]).astype(jnp.bfloat16)

    for m in range(tiles - 1):
        with scope(f"fin{m}"):
            if m:
                phase2_done(m)
        with scope(f"out{m}"):
            finish(m)

    @pl.when(row == 0)
    def _():
        out_ref[0] = whole(s0_ref)

    @pl.when(row == 1)
    def _():
        out_ref[0] = whole(s1_ref)

    for part in range(2):
        for step in range(1, far + 1):
            drain(ring_block(part, step, 1), up_send.at[part, step - 1])
            drain(ring_block(part, step, -1), down_send.at[part, step - 1])
        ring_paired(part, pair_send)
    for m in range(tiles):
        drain(a_refs[m].at[pl.ds(0, cols - 1)], p1_send.at[m])
        if m < tiles - 1:
            drain(t_refs[m].at[pl.ds(0, cols - 1)], p2_send.at[m])

    def pieces(n):
        return c_ref.at[0, pl.ds(0, n * piece), :]

    for root in range(2):
        near_z = (x == root % wide) & (row != root)
        near_x = (z == root // wide) & (row != root)

        @pl.when(row == root)
        def _():
            drain(pieces(rows - 1), sc_send.at[root])

        for near, sem, count, each in (
            (near_z, gz_send, deep - 1, 1), (near_x, gx_send, wide - 1, deep),
        ):
            if count > 1:
                @pl.when(near)
                def _():
                    drain(pieces((count - 1) * each), sem.at[root])

            @pl.when(jnp.logical_not(near))
            def _():
                drain(pieces(count * each), sem.at[root])

    last = tiles - 1
    with scope("fin2"):
        phase2_done(last)
    with scope("out2"):
        finish(last)
    drain(t_refs[last].at[pl.ds(0, cols - 1)], p2_send.at[last])


def body(rows, cols, wide, lower, rhs, tile_map):
    rhs = rhs[0]
    panels = jnp.transpose(lower[0], (0, 2, 3, 1))
    tiles, tile, width = rhs.shape
    slab = tile // cols
    far = cols // 4
    vmem = pl.BlockSpec(memory_space=pltpu.VMEM)
    dma = pltpu.SemaphoreType.DMA
    lanes = [pltpu.VMEM((cols, slab, width), jnp.bfloat16) for _ in range(6)]
    out = pl.pallas_call(
        functools.partial(kernel, rows, cols, wide),
        name="solve_step",
        out_shape=pltpu.VMEM(rhs.shape, jnp.bfloat16),
        in_specs=[pl.BlockSpec(memory_space=pl.ANY)] * 3,
        out_specs=vmem,
        scratch_shapes=[
            pltpu.SMEM(tile_map.shape, jnp.int32),
            pltpu.VMEM(rhs.shape, jnp.bfloat16),
            pltpu.VMEM(panels.shape, jnp.bfloat16),
            *lanes,
            pltpu.VMEM((tiles, tile, width), jnp.bfloat16),
            pltpu.VMEM((tiles, 2, tile, tile), jnp.bfloat16),
            pltpu.VMEM((tiles, 2, tile, tile), jnp.bfloat16),
            pltpu.VMEM((rows // wide, wide, tile // rows, width), jnp.bfloat16),
            pltpu.VMEM((rows // wide, wide, tile // rows, width), jnp.bfloat16),
            pltpu.VMEM((tiles, tile, width), jnp.float32),
            pltpu.VMEM((tile, tile), jnp.float32),
            pltpu.VMEM((tile // BLOCK, BLOCK, BLOCK), jnp.float32),
            pltpu.VMEM((tile, width), jnp.float32),
            dma((tiles,)), dma((tiles,)), dma((tiles,)), dma((tiles,)),
            dma((2, far)), dma((2, far)), dma((2, far)), dma((2, far)),
            dma((2,)), dma((2,)),
            dma((2,)), dma((2,)), dma((2,)), dma((2,)), dma((2,)), dma((2,)),
            dma((4,)), pltpu.SemaphoreType.REGULAR((2,)),
            pltpu.SemaphoreType.REGULAR, pltpu.SemaphoreType.REGULAR,
        ],
        compiler_params=pltpu.CompilerParams(
            collective_id=0, has_side_effects=True, vmem_limit_bytes=VMEM_BYTES
        ),
    )(tile_map, rhs, panels)
    return out[None]


def solution(mesh):
    rows, cols = mesh.shape["row"], mesh.shape["col"]
    wide = 4 if rows % 16 == 0 else 2
    return jax.shard_map(
        functools.partial(body, rows, cols, wide),
        mesh=mesh,
        in_specs=(P("row", None, None, None, "col"), P("row", None, None, "col"), P()),
        out_specs=P("row", None, None, "col"),
        check_vma=False,
    )
```
